32 devices in a mesh: dp: 2 (over x), expert: 16 (over z, y, core).
Axes of the slice: x: 2, y: 2, z: 4, core: 2. Of those that a mesh axis runs over, the one named last changes fastest.
Arguments:
- hidden: bfloat16 [2, 1024, 2, 2048], P('dp', 'expert'), may hold values from -6 to 6
- queries: bfloat16 [2, 1024, 2, 4096], P('dp', 'expert'), may hold values from -45 to 45
- latents: bfloat16 [2, 1024, 2, 512], P('dp', 'expert'), may hold values from -165 to 165
- mem_latents: bfloat16 [2, 32, 2, 512], P('dp'), may hold values from -6 to 6
- lengths: int32 [2, 2], P('dp'), may hold values from 512 to 1024
- ids: int32 [2, 1024, 2, 6], P('dp', 'expert'), may hold values from 0 to 15, all different within a row; in each aligned block of 128 rows (0 to 127, 128 to 255, ..., all dimensions but the last counted through in order) at most 50 rows name the same one
- gates: bfloat16 [2, 1024, 2, 6], P('dp', 'expert'), may hold values from 0.049804688 to 0.5
- norm_gain: bfloat16 [2048], replicated, may hold values from 0.25 to 1.75
- w_uv: bfloat16 [8, 512, 128], P('dp'), may hold values from -0.25 to 0.25
- w_out: bfloat16 [1024, 2048], P('dp'), may hold values from -0.1875 to 0.1875
- w_gate: bfloat16 [16, 2048, 704], P('expert'), may hold values from -0.125 to 0.125
- w_up: bfloat16 [16, 2048, 704], P('expert'), may hold values from -0.125 to 0.125
- w_down: bfloat16 [16, 704, 2048], P('expert'), may hold values from -0.21875 to 0.21875
Outputs:
- layer_out: bfloat16 [2, 1024, 2, 2048], P('dp', 'expert')
The draws below stay inside these ranges and needn't reach their ends.
Inputs may be any that keep to these rules, and one draw needn't show every extreme that they name: `ids`: each row names 6 different experts; the rows of one device (aligned blocks of 128 rows in the order of the leading dimensions) name any one expert at most 50 times, a bound that some block reaches.
All inputs are finite; a program needn't handle non-finite values.
Results may differ from the reference program's by a relative error of at most 0.007.
Values may be sent and summed in bfloat16 or wider, within the bound.
No kernel may reach another device: no remote copies, remote signals or barrier semaphores. Data moves between devices by JAX's collectives and lax.ppermute only.
A program may use at most 128 MiB of HBM per device.

```python
import math
import jax
import jax.numpy as jnp
import numpy as np
from jax import lax

D = 2048
HEADS = 8
LAT = 512
VDIM = 128
FF = 704
TOPK = 6
MEM = 32
SEQS = 2
SEG = 1024
TOK_DEV = 128
EXPERTS = 16
CAP = 50
N_DP = 2
N_EXPERT = 16


def draw_latents(key, part):
    entries = jnp.clip(jax.random.normal(jax.random.fold_in(key, 1), (N_DP, SEG, SEQS, LAT), jnp.float32), -6.0, 6.0)
    return entries.astype(jnp.bfloat16)


def draw_queries(key, part):
    full_shape = (N_DP, SEG, SEQS, HEADS, LAT)
    entries = 0.5 * jnp.clip(jax.random.normal(jax.random.fold_in(key, 3), full_shape, jnp.float32), -6.0, 6.0)
    return entries.reshape(N_DP, SEG, SEQS, HEADS * LAT).astype(jnp.bfloat16)


def set_ends(drawn, rng, low, largest):
    spot = [jax.random.randint(jax.random.fold_in(rng, axis), (), 0, length) for axis, length in enumerate(drawn.shape)]
    longest = drawn.shape.index(max(drawn.shape))
    neighbour = spot[:longest] + [(spot[longest] + 1) % drawn.shape[longest]] + spot[longest + 1:]
    return drawn.at[tuple(spot)].set(low).at[tuple(neighbour)].set(largest)


def steps_of(key, extent, shards, least, high):
    level, own = 1.0, jax.random.fold_in(key, 6)
    for dim, parts in shards:
        heights = jnp.exp(jax.random.uniform(jax.random.fold_in(own, dim), (parts,), jnp.float32, least / len(shards), high / len(shards)))
        level = level * jnp.repeat(heights, extent[dim] // parts).reshape([-1 if axis == dim else 1 for axis in range(len(extent))])
    return level


def routed_block(own_key, own, number, rows, number_of, top, most, slope):
    ranking = jax.random.permutation(own_key, number_of)
    crowded, ordinary = portions_of(number_of, rows * top, most, slope, True), portions_of(number_of, rows * top, most, slope, False)
    places = jnp.arange(number_of)

    def named(sizes, offset_by):
        used = int((sizes > 0).sum())
        fixed = max(1, used // 4)
        moved = fixed + (places - fixed + offset_by * (used - fixed)) % max(1, number_of - fixed)
        return jnp.zeros((number_of,), jnp.int32).at[ranking[jnp.where(places < fixed, places, moved)]].set(jnp.asarray(sizes, jnp.int32))

    sizes = jnp.where(number % 4 == 0, named(crowded, number // 4), named(ordinary, number - number // 4 - 1))
    mixed = jax.random.permutation(jax.random.fold_in(own, 3), number_of)
    giver, sink = mixed[0:number_of // 2 * 2:2], mixed[1:number_of // 2 * 2:2]
    margin = jnp.minimum(sizes[giver] - 1, most - sizes[sink]) // 2
    margin = jnp.where((giver == ranking[0]) | (sink == ranking[0]) | (sizes[sink] == 0), 0, jnp.maximum(margin, 0))
    moved = jax.random.randint(jax.random.fold_in(own, 4), (number_of // 2,), 0, 1 << 20) % (margin + 1)
    sizes = sizes.at[giver].add(-moved).at[sink].add(moved)
    labels = jnp.searchsorted(jnp.cumsum(sizes), jnp.arange(rows * top), side="right").astype(jnp.int32)
    table = labels.reshape(top, rows).T
    table = table[jax.random.permutation(jax.random.fold_in(own, 1), rows)]
    offset_by = jax.random.randint(jax.random.fold_in(own, 2), (rows, 1), 0, top)
    return jnp.take_along_axis(table, (jnp.arange(top)[None, :] + offset_by) % top, axis=1)


def portions_of(number_of, total, reach, skew, full):
    weights = [(1 << 20) // math.isqrt(grade ** skew) + 1 for grade in range(1, number_of + 1)]
    largest = reach if full else min(reach, max(-(-total // number_of), total * weights[0] // sum(weights)))
    least = 1 if total - largest >= number_of - 1 else 0
    given, surplus = [largest] + [least] * (number_of - 1), total - largest - least * (number_of - 1)
    while surplus > 0:
        candidates = [i for i in range(1, number_of) if given[i] < largest] or [i for i in range(1, number_of) if given[i] < reach]
        pool, budget = sum([weights[i] for i in candidates]), surplus
        for i in candidates:
            extra = min(reach - given[i], max(1, budget * weights[i] // pool), surplus)
            given[i] = given[i] + extra
            surplus = surplus - extra
    return np.array(given)


def scatter_about(key, shape, scale, most, cuts=(), held_as=jnp.bfloat16):
    values = jax.random.normal(key, shape, jnp.float32) * scale
    if len(cuts) > 0:
        values = steps_of(key, shape, cuts, -0.22, 0.18) * values
    return jnp.clip(values, min=-most, max=most).astype(held_as)


def setup_inputs(seed: int = 0) -> dict:
    arg_keys = jax.random.split(jax.random.key(seed), 14)
    hidden = scatter_about(arg_keys[0], (N_DP, SEG, SEQS, D), 1.0, 6.0, ((0, 2), (1, 16)))
    queries = draw_queries(jax.random.fold_in(arg_keys[13], 71), 0)
    latents = draw_latents(jax.random.fold_in(arg_keys[13], 71), 0)
    mem_latents = scatter_about(arg_keys[3], (N_DP, MEM, SEQS, LAT), 1.0, 6.0, ((0, 2),))
    lengths = set_ends(jax.random.randint(arg_keys[4], (N_DP, SEQS), SEG // 2, SEG + 1), jax.random.fold_in(arg_keys[4], 1), SEG // 2, SEG).astype(jnp.int32)
    ids_keys = jax.random.split(jax.random.fold_in(arg_keys[5], 1), N_DP * SEG * SEQS // TOK_DEV)
    ids_turns = jax.random.permutation(jax.random.fold_in(arg_keys[5], 3), N_DP * SEG * SEQS // TOK_DEV)
    ids = jax.vmap(lambda own, number: routed_block(jax.random.fold_in(arg_keys[5], 2), own, number, TOK_DEV, EXPERTS, TOPK, CAP, 2))(ids_keys, ids_turns).reshape((N_DP, SEG, SEQS, TOPK))
    gates = jnp.clip(jnp.exp(math.log(0.5) - 2.306499 * jax.random.uniform(arg_keys[6], (N_DP, SEG, SEQS, TOPK), jnp.float32) ** steps_of(arg_keys[6], (N_DP, SEG, SEQS, TOPK), ((0, 2), (1, 16)), -0.2, 0.2)), 0.049804688, 0.5).astype(jnp.bfloat16)
    norm_gain = jnp.clip(1.0 + 0.15 * jax.random.normal(arg_keys[7], (D,), jnp.float32), 0.25, 1.75).astype(jnp.bfloat16)
    w_uv = scatter_about(arg_keys[8], (HEADS, LAT, VDIM), LAT ** -0.5, 0.25, ((0, 2),))
    w_out = scatter_about(arg_keys[9], (HEADS * VDIM, D), (HEADS * VDIM) ** -0.5, 0.1875, ((0, 2),))
    w_gate = scatter_about(arg_keys[10], (EXPERTS, D, FF), D ** -0.5, 0.125, ((0, 16),))
    w_up = scatter_about(arg_keys[11], (EXPERTS, D, FF), D ** -0.5, 0.125, ((0, 16),))
    w_down = scatter_about(arg_keys[12], (EXPERTS, FF, D), FF ** -0.5, 0.21875, ((0, 16),))
    return {"hidden": hidden, "queries": queries, "latents": latents, "mem_latents": mem_latents, "lengths": lengths, "ids": ids, "gates": gates, "norm_gain": norm_gain, "w_uv": w_uv, "w_out": w_out, "w_gate": w_gate, "w_up": w_up, "w_down": w_down}


score_scale = 192.0 ** (-0.5)
norm_eps = 1e-06

def attend_one(query_rows, seg_latent, mem_latent, seq_limit):
    key_rows = jnp.concatenate([mem_latent, seg_latent], axis=0).astype(jnp.float32)
    scores = jnp.einsum('ihl,jl->hij', query_rows.astype(jnp.float32), key_rows) * score_scale
    query_pos = jnp.arange(SEG, dtype=jnp.int32)
    seg_visible = (query_pos[None, :] <= query_pos[:, None]) & (query_pos[None, :] < seq_limit)
    visible = jnp.concatenate([jnp.ones((SEG, MEM), dtype=bool), seg_visible], axis=1)
    scores = jnp.where(visible[None], scores, -jnp.inf)
    row_top = lax.optimization_barrier(jnp.max(scores, axis=2))
    weights = jnp.exp(scores - row_top[..., None])
    exp_total = lax.optimization_barrier(jnp.sum(weights, axis=2))
    rounded = lax.optimization_barrier(weights.astype(jnp.bfloat16)).astype(jnp.float32)
    attended = jnp.einsum('hij,jl->ihl', rounded, key_rows) / jnp.transpose(exp_total)[..., None]
    return attended.astype(jnp.bfloat16)

def reference(hidden, queries, latents, mem_latents, lengths, ids, gates, norm_gain, w_uv, w_out, w_gate, w_up, w_down):
    batch = N_DP * SEQS
    query_all = queries.reshape(N_DP, SEG, SEQS, HEADS, LAT).transpose(0, 2, 1, 3, 4).reshape(batch, SEG, HEADS, LAT)
    seg_all = latents.transpose(0, 2, 1, 3).reshape(batch, SEG, LAT)
    mem_all = mem_latents.transpose(0, 2, 1, 3).reshape(batch, MEM, LAT)
    limits = lengths.reshape(batch)
    attended = lax.map(lambda item: attend_one(item[0], item[1], item[2], item[3]), (query_all, seg_all, mem_all, limits))
    values = jnp.einsum('bihl,hlv->bihv', attended.astype(jnp.float32), w_uv.astype(jnp.float32)).astype(jnp.bfloat16)
    attn_out = jnp.dot(values.reshape(batch * SEG, HEADS * VDIM), w_out, preferred_element_type=jnp.float32)
    attn_out = attn_out.reshape(N_DP, SEQS, SEG, D).transpose(0, 2, 1, 3)
    residual = hidden.astype(jnp.float32) + attn_out
    mean_square = lax.optimization_barrier(jnp.mean(residual * residual, axis=-1, keepdims=True))
    normed = (residual * lax.rsqrt(mean_square + norm_eps) * norm_gain.astype(jnp.float32)).astype(jnp.bfloat16)
    row_total = N_DP * SEG * SEQS
    flat_normed = normed.reshape(row_total, D)
    flat_ids = ids.reshape(row_total * TOPK)
    flat_gates = gates.reshape(row_total * TOPK).astype(jnp.float32)
    reach_rows = N_DP * N_EXPERT * CAP

    def per_expert(running, item):
        gate_w, up_w, down_w, expert_id = item
        matches = flat_ids == expert_id
        picked = jnp.nonzero(matches, size=reach_rows, fill_value=0)[0].astype(jnp.int32)
        is_live = jnp.arange(reach_rows, dtype=jnp.int32) < jnp.sum(matches.astype(jnp.int32))
        token_index = (picked // TOPK).astype(jnp.int32)
        picked_rows = flat_normed[token_index]
        gate_h = jnp.dot(picked_rows, gate_w, preferred_element_type=jnp.float32)
        up_h = jnp.dot(picked_rows, up_w, preferred_element_type=jnp.float32)
        act = (jax.nn.silu(gate_h) * up_h).astype(jnp.bfloat16)
        out_rows = jnp.dot(act, down_w, preferred_element_type=jnp.float32).astype(jnp.bfloat16)
        out_rows = lax.optimization_barrier(out_rows).astype(jnp.float32)
        scale_w = jnp.where(is_live, flat_gates[picked], jnp.float32(0.0))
        running = running.at[token_index].add(scale_w[:, None] * out_rows)
        return (running, None)
    start_acc = jnp.zeros((row_total, D), jnp.float32)
    routed, unused = lax.scan(per_expert, start_acc, (w_gate, w_up, w_down, jnp.arange(EXPERTS, dtype=jnp.int32)))
    layer_out = residual + routed.reshape(N_DP, SEG, SEQS, D)
    return layer_out.astype(jnp.bfloat16)
```

```python
import jax
import jax.numpy as jnp
from jax import lax
from jax.sharding import PartitionSpec as P

score_scale = 192.0 ** (-0.5)
norm_eps = 1e-06


def flip(value, mask, size):
    return lax.ppermute(value, "expert", [(i, i ^ mask) for i in range(size)])


def gather_latents(own, size):
    pieces = {0: own}
    quarter = size // 4
    for mask in (2 * quarter, 3 * quarter, quarter):
        pieces[mask] = flip(own, mask, size)
    step = quarter // 2
    while step:
        for mask in list(pieces):
            pieces[mask ^ step] = flip(pieces[mask], step, size)
        step //= 2
    return pieces


def fetch_weights(w_uv, w_out, core, size):
    dp = lax.axis_size("dp")
    heads = w_uv.shape[0]
    half = heads // 2
    width = w_out.shape[0] // heads
    parts = []
    for turn in range(1, dp):
        source = [((i + turn) % dp, i) for i in range(dp)]
        uv_half = lax.dynamic_slice_in_dim(w_uv, core * half, half, 0)
        out_half = lax.dynamic_slice_in_dim(w_out, core * half * width, half * width, 0)
        uv_got = lax.ppermute(uv_half, "dp", source)
        out_got = lax.ppermute(out_half, "dp", source)
        parts.append((uv_got, out_got))
        parts.append((flip(uv_got, 1, size), flip(out_got, 1, size)))
    return parts


def order_heads(query_rows, core, heads_here):
    dp = lax.axis_size("dp")
    index = lax.axis_index("dp")
    half = heads_here // 2
    blocks = [lax.dynamic_slice_in_dim(query_rows, index * heads_here, heads_here, 0)]
    for turn in range(1, dp):
        first = ((index + turn) % dp) * heads_here
        blocks.append(lax.dynamic_slice_in_dim(query_rows, first + core * half, half, 0))
        blocks.append(lax.dynamic_slice_in_dim(query_rows, first + (1 - core) * half, half, 0))
    return jnp.concatenate(blocks, axis=0)


def route(ids, gates, experts, capacity):
    rows = ids.shape[0]
    hit = ids[None, :, :] == experts[:, None, None]
    named = jnp.any(hit, axis=2)
    weight = jnp.sum(jnp.where(hit, gates[None].astype(jnp.float32), 0.0), axis=2)
    row = jnp.arange(rows, dtype=jnp.int32)
    earlier = (row[:, None] < row[None, :]).astype(jnp.bfloat16)
    rank = jnp.dot(named.astype(jnp.bfloat16), earlier, preferred_element_type=jnp.float32)
    slot = jnp.where(named, rank.astype(jnp.int32), -1)
    place = slot[:, None, :] == jnp.arange(capacity, dtype=jnp.int32)[None, :, None]
    placing = place.astype(jnp.bfloat16)
    mixing = jnp.where(place, weight[:, None, :], 0.0).astype(jnp.bfloat16)
    count = experts.shape[0] * capacity
    return placing.reshape(count, rows), mixing.reshape(count, rows)


def shards(
    hidden,
    queries,
    latents,
    mem_latents,
    lengths,
    ids,
    gates,
    norm_gain,
    w_uv,
    w_out,
    w_gate,
    w_up,
    w_down,
):
    local_len, seq_count, model_width = hidden.shape[1:]
    latent_dim = latents.shape[3]
    head_count = queries.shape[3] // latent_dim
    heads_here = w_uv.shape[0]
    value_dim = w_uv.shape[2]
    row_count = local_len * seq_count
    size = lax.axis_size("expert")
    shard_index = lax.axis_index("expert")
    core = shard_index & 1
    half_size = size // 2
    own_pos = shard_index * local_len + jnp.arange(local_len, dtype=jnp.int32)

    pieces = gather_latents(jnp.transpose(latents[0], (1, 0, 2)), size)
    parts = fetch_weights(w_uv, w_out, core, size)
    top_count = ids.shape[3]
    flat_ids = ids[0].reshape(row_count, top_count)
    flat_gates = gates[0].reshape(row_count, top_count)
    far_ids = flip(flat_ids, half_size, size)
    far_gates = flip(flat_gates, half_size, size)

    query_rows = queries[0].reshape(local_len, seq_count, head_count, latent_dim)
    query_rows = order_heads(jnp.transpose(query_rows, (2, 1, 0, 3)), core, heads_here)
    query_rows = jnp.transpose(query_rows, (1, 0, 2, 3)).reshape(
        seq_count, head_count * local_len, latent_dim
    )
    masks = sorted(pieces)
    keys = jnp.concatenate([jnp.transpose(mem_latents[0], (1, 0, 2))] + [pieces[m] for m in masks], axis=1)
    mem_len = mem_latents.shape[1]
    in_piece = jnp.arange(local_len, dtype=jnp.int32)
    seg_pos = ((shard_index ^ jnp.array(masks, jnp.int32))[:, None] * local_len + in_piece).reshape(-1)
    key_pos = jnp.concatenate([jnp.full((mem_len,), -1, jnp.int32), seg_pos])
    scores = (
        jnp.einsum("sql,skl->sqk", query_rows, keys, preferred_element_type=jnp.float32) * score_scale
    ).reshape(seq_count, head_count, local_len, -1)
    causal = key_pos[None, :] <= own_pos[:, None]
    inside = key_pos[None, :] < lengths[0][:, None]
    visible = causal[None, None, :, :] & inside[:, None, None, :]
    scores = jnp.where(visible, scores, -jnp.inf)
    weights = jnp.exp(scores - jnp.max(scores, axis=3, keepdims=True))
    total = jnp.sum(weights, axis=3)
    attended = jnp.einsum(
        "shtk,skl->shtl", weights.astype(jnp.bfloat16), keys, preferred_element_type=jnp.float32
    )
    attended = (attended / total[..., None]).astype(jnp.bfloat16)

    attn_out = None
    at = 0
    for uv_part, out_part in [(w_uv, w_out)] + parts:
        count = uv_part.shape[0]
        values = jnp.einsum(
            "shtl,hlv->tshv", attended[:, at : at + count], uv_part, preferred_element_type=jnp.float32
        ).astype(jnp.bfloat16)
        term = jnp.dot(
            values.reshape(row_count, count * value_dim), out_part, preferred_element_type=jnp.float32
        )
        attn_out = term if attn_out is None else attn_out + term
        at += count
    residual = hidden[0].reshape(row_count, model_width).astype(jnp.float32) + attn_out
    mean_square = jnp.mean(residual * residual, axis=-1, keepdims=True)
    normed = (residual * lax.rsqrt(mean_square + norm_eps) * norm_gain.astype(jnp.float32)).astype(
        jnp.bfloat16
    )

    experts_here = w_gate.shape[0]
    expert_count = size * experts_here
    capacity = min(row_count, row_count * top_count // expert_count + 2)
    capacity = -(-capacity // 8) * 8
    index_here = shard_index % half_size
    first_expert = shard_index - index_here
    owners = first_expert + (index_here ^ jnp.arange(half_size, dtype=jnp.int32))
    owned = (owners[:, None] * experts_here + jnp.arange(experts_here, dtype=jnp.int32)).reshape(-1)
    block = experts_here * capacity
    near_place, near_mix = route(flat_ids, flat_gates, owned, capacity)
    far_place, far_mix = route(far_ids, far_gates, owned, capacity)

    def swap(blocks):
        return jnp.concatenate(
            [blocks[:block]]
            + [flip(blocks[m * block : (m + 1) * block], m, size) for m in range(1, half_size)],
            axis=0,
        )

    def send(placing, rows):
        return swap(jnp.dot(placing, rows, preferred_element_type=jnp.float32).astype(jnp.bfloat16))

    def experts(incoming):
        rows = incoming.reshape(half_size, experts_here, capacity, model_width)
        gate_h = jnp.einsum("necd,edf->necf", rows, w_gate, preferred_element_type=jnp.float32)
        up_h = jnp.einsum("necd,edf->necf", rows, w_up, preferred_element_type=jnp.float32)
        act = (jax.nn.silu(gate_h) * up_h).astype(jnp.bfloat16)
        out = jnp.einsum("necf,efd->necd", act, w_down, preferred_element_type=jnp.float32)
        return out.astype(jnp.bfloat16).reshape(half_size * block, model_width)

    def mix(mixing, returned):
        return lax.dot_general(
            mixing, returned, (((0,), (0,)), ((), ())), preferred_element_type=jnp.float32
        )

    far_rows = flip(normed, half_size, size)
    near_in = send(near_place, normed)
    far_in = send(far_place, far_rows)
    near_out = experts(near_in)
    far_out = experts(far_in)
    far_sum = mix(far_mix, swap(far_out)).astype(jnp.bfloat16)
    other_sum = flip(far_sum, half_size, size)
    near_sum = mix(near_mix, swap(near_out))
    layer_out = (residual + near_sum + other_sum.astype(jnp.float32)).astype(jnp.bfloat16)
    return layer_out.reshape(1, local_len, seq_count, model_width)


def solution(mesh):
    return jax.shard_map(
        shards,
        mesh=mesh,
        in_specs=(
            P("dp", "expert", None, None),
            P("dp", "expert", None, None),
            P("dp", "expert", None, None),
            P("dp", None, None, None),
            P("dp", None),
            P("dp", "expert", None, None),
            P("dp", "expert", None, None),
            P(),
            P("dp", None, None),
            P("dp", None),
            P("expert", None, None),
            P("expert", None, None),
            P("expert", None, None),
        ),
        out_specs=P("dp", "expert", None, None),
        check_vma=False,
    )
```

```python
import functools

import jax
import jax.numpy as jnp
from jax import lax
from jax.experimental import pallas as pl
from jax.experimental.pallas import tpu as pltpu
from jax.sharding import PartitionSpec as P

score_scale = 192.0 ** (-0.5)
norm_eps = 1e-06


bf16, f32, i32 = jnp.bfloat16, jnp.float32, jnp.int32
VMEM = pl.BlockSpec(memory_space=pltpu.VMEM)
SMEM = pl.BlockSpec(memory_space=pltpu.SMEM)
ANY = pl.BlockSpec(memory_space=pl.ANY)


def flip(value, mask, size):
    return lax.ppermute(value, "expert", [(i, i ^ mask) for i in range(size)])


def call(body, name, in_specs, outs, operands, flops=0, scratch=()):
    return pl.pallas_call(
        body,
        name=name,
        in_specs=in_specs,
        out_specs=[VMEM] * len(outs),
        out_shape=[jax.ShapeDtypeStruct(s, d) for s, d in outs],
        scratch_shapes=list(scratch),
        compiler_params=pltpu.CompilerParams(vmem_limit_bytes=56 * 1024 * 1024),
        cost_estimate=pl.CostEstimate(flops=flops, bytes_accessed=0, transcendentals=0),
    )(*operands)


def gather_latents(own, size):
    pieces = {0: own}
    quarter = size // 4
    for mask in (2 * quarter, 3 * quarter, quarter):
        pieces[mask] = flip(own, mask, size)
    step = quarter // 2
    while step:
        for mask in list(pieces):
            pieces[mask ^ step] = flip(pieces[mask], step, size)
        step //= 2
    return [pieces[m] for m in range(size)]


def fetch_weights(w_uv, w_out, core, size):
    dp = lax.axis_size("dp")
    heads = w_uv.shape[0]
    half = heads // 2
    width = w_out.shape[0] // heads
    uv_half = lax.dynamic_slice_in_dim(w_uv, core * half, half, 0)
    out_half = lax.dynamic_slice_in_dim(w_out, core * half * width, half * width, 0)
    parts = [(w_uv, w_out)]
    for turn in range(1, dp):
        source = [((i + turn) % dp, i) for i in range(dp)]
        uv_got = lax.ppermute(uv_half, "dp", source)
        out_got = lax.ppermute(out_half, "dp", source)
        parts.append((uv_got, out_got))
        parts.append((flip(uv_got, 1, size), flip(out_got, 1, size)))
    return parts


def head_order(core, heads):
    dp = lax.axis_size("dp")
    index = lax.axis_index("dp")
    half = heads // 2
    order = [index * heads + h for h in range(heads)]
    for turn in range(1, dp):
        first = ((index + turn) % dp) * heads
        order += [first + core * half + h for h in range(half)]
        order += [first + (1 - core) * half + h for h in range(half)]
    return jnp.stack(order).astype(i32)


def attend_body(size, local_len, seq_count, latent, heads, group, *refs):
    info, lengths, queries, memory = refs[:4]
    pieces = refs[4 : 4 + size]
    out, keys, rows = refs[4 + size :]
    seg_len = size * local_len
    total_len = seg_len + memory.shape[0]
    shift = local_len.bit_length() - 1
    index = info[0]
    at = lax.broadcasted_iota(i32, (local_len, total_len), 1)
    row = lax.broadcasted_iota(i32, (local_len, total_len), 0)
    pos = jnp.left_shift(jnp.bitwise_xor(jnp.right_shift(at, shift), index), shift) + jnp.bitwise_and(
        at, local_len - 1
    )
    pos = jnp.where(at < seg_len, pos, -1)
    causal = pos <= index * local_len + row
    for s in range(seq_count):
        cols = pl.ds(s * latent, latent)
        for m in range(size):
            keys[pl.ds(m * local_len, local_len), :] = pieces[m][:, cols]
        keys[pl.ds(seg_len, memory.shape[0]), :] = memory[:, cols]
        bias = jnp.where(causal & (pos < lengths[0, s]), 0.0, -jnp.inf)
        bias = jnp.concatenate([bias] * group, axis=0)
        for first in range(0, heads, group):
            for h in range(group):
                rows[pl.ds(h * local_len, local_len), :] = queries[
                    :, pl.ds((s * heads + first + h) * latent, latent)
                ]
            scores = lax.dot_general(
                rows[...], keys[...], (((1,), (1,)), ((), ())), preferred_element_type=f32
            )
            scores = scores * score_scale + bias
            top = jnp.max(scores, axis=1, keepdims=True)
            weights = jnp.exp(scores - top)
            total = jnp.sum(weights, axis=1, keepdims=True)
            got = jnp.dot(weights.astype(bf16), keys[...], preferred_element_type=f32) / total
            got = got.astype(bf16)
            for h in range(group):
                out[pl.ds(s * local_len, local_len), pl.ds((first + h) * latent, latent)] = got[
                    h * local_len : (h + 1) * local_len
                ]


def routes(info, table, top, half, capacity):
    rows = table.shape[0]
    table = table[...]
    names, gates = table[:, :top], table[:, top : 2 * top]
    lane = lax.broadcasted_iota(i32, (rows, half), 1)
    named = jnp.zeros((rows, half), f32)
    weight = jnp.zeros((rows, half), f32)
    for m in range(half):
        hit = names == info[2 + m].astype(f32)
        count = jnp.sum(jnp.where(hit, 1.0, 0.0), axis=1, keepdims=True)
        share = jnp.sum(jnp.where(hit, gates, 0.0), axis=1, keepdims=True)
        named = jnp.where(lane == m, count, named)
        weight = jnp.where(lane == m, share, weight)
    r = lax.broadcasted_iota(i32, (rows, rows), 0)
    c = lax.broadcasted_iota(i32, (rows, rows), 1)
    upto = jnp.where(c <= r, 1.0, 0.0).astype(bf16)
    rank = named * jnp.dot(upto, named.astype(bf16), preferred_element_type=f32)
    wide = half * capacity
    col = lax.broadcasted_iota(i32, (half, wide), 1)
    start = lax.broadcasted_iota(i32, (half, wide), 0) * capacity
    inside = (col >= start) & (col < start + capacity)
    spread = jnp.where(inside, 1.0, 0.0).astype(bf16)
    slot = jnp.sum(jnp.where(inside, col - start + 1, 0), axis=0, keepdims=True).astype(f32)
    rank = jnp.dot(rank.astype(bf16), spread, preferred_element_type=f32)
    weight = jnp.dot(weight.astype(bf16), spread, preferred_element_type=f32)
    place = rank == slot
    return jnp.where(place, 1.0, 0.0).astype(bf16), jnp.where(place, weight, 0.0).astype(bf16)


def put_blocks(placing, rows, blocks, capacity):
    sent = lax.dot_general(placing, rows, (((0,), (0,)), ((), ())), preferred_element_type=f32).astype(bf16)
    for m, block in enumerate(blocks):
        block[...] = sent[m * capacity : (m + 1) * capacity]


def middle_body(parts, half, capacity, top, local_len, seq_count, latent, *refs):
    info, order, attended, hidden, gain, table = refs[:6]
    maps = refs[6 : 6 + 2 * parts]
    residual, normed, mixing = refs[6 + 2 * parts : 9 + 2 * parts]
    blocks = refs[9 + 2 * parts :]
    width = gain.shape[1]
    acc = jnp.concatenate([hidden[:, s * width : (s + 1) * width] for s in range(seq_count)], axis=0).astype(f32)
    slot = 0
    for part in range(parts):
        uv, proj = maps[2 * part], maps[2 * part + 1]
        values = []
        for h in range(uv.shape[0]):
            at = pl.multiple_of(order[slot] * latent, latent)
            got = jnp.dot(attended[:, pl.ds(at, latent)], uv[h], preferred_element_type=f32)
            values.append(got.astype(bf16))
            slot += 1
        acc = acc + jnp.dot(jnp.concatenate(values, axis=1), proj[...], preferred_element_type=f32)
    residual[...] = acc
    mean_square = jnp.mean(acc * acc, axis=1, keepdims=True)
    scaled = (acc * lax.rsqrt(mean_square + norm_eps) * gain[...].astype(f32)).astype(bf16)
    normed[...] = scaled
    placing, mixed = routes(info, table, top, half, capacity)
    mixing[...] = mixed
    put_blocks(placing, scaled, blocks, capacity)


def far_body(half, capacity, top, info, table, rows, mixing, *blocks):
    placing, mixed = routes(info, table, top, half, capacity)
    mixing[...] = mixed
    put_blocks(placing, rows[...], blocks, capacity)


def expert_body(half, capacity, *refs):
    gate_hbm, up_hbm, down_hbm = refs[:3]
    taken = refs[3 : 3 + half]
    given = refs[3 + half : 3 + 2 * half]
    gate, up, down, rows, sems = refs[3 + 2 * half :]
    copies = [
        pltpu.make_async_copy(source.at[0], target, sems.at[i])
        for i, (source, target) in enumerate(((gate_hbm, gate), (up_hbm, up), (down_hbm, down)))
    ]
    for copy in copies:
        copy.start()
    for m in range(half):
        rows[pl.ds(m * capacity, capacity), :] = taken[m][...]
    copies[0].wait()
    gate_h = jnp.dot(rows[...], gate[...], preferred_element_type=f32)
    copies[1].wait()
    up_h = jnp.dot(rows[...], up[...], preferred_element_type=f32)
    act = (gate_h / (1.0 + jnp.exp(-gate_h)) * up_h).astype(bf16)
    copies[2].wait()
    out = jnp.dot(act, down[...], preferred_element_type=f32).astype(bf16)
    for m in range(half):
        given[m][...] = out[m * capacity : (m + 1) * capacity]


def mix_body(half, capacity, mixing, *refs):
    taken, out, rows = refs[:half], refs[half], refs[half + 1]
    for m in range(half):
        rows[pl.ds(m * capacity, capacity), :] = taken[m][...]
    out[...] = jnp.dot(mixing[...], rows[...], preferred_element_type=f32).astype(bf16)


def last_body(half, capacity, local_len, seq_count, mixing, residual, other, *refs):
    taken, out, rows = refs[:half], refs[half], refs[half + 1]
    for m in range(half):
        rows[pl.ds(m * capacity, capacity), :] = taken[m][...]
    total = jnp.dot(mixing[...], rows[...], preferred_element_type=f32)
    total = (residual[...] + total + other[...].astype(f32)).astype(bf16)
    width = total.shape[1]
    for s in range(seq_count):
        out[:, s * width : (s + 1) * width] = total[s * local_len : (s + 1) * local_len]


def shards(
    hidden,
    queries,
    latents,
    mem_latents,
    lengths,
    ids,
    gates,
    norm_gain,
    w_uv,
    w_out,
    w_gate,
    w_up,
    w_down,
):
    local_len, seq_count, width = hidden.shape[1:]
    latent = latents.shape[3]
    heads = queries.shape[3] // latent
    rows = local_len * seq_count
    top = ids.shape[3]
    size = lax.axis_size("expert")
    index = lax.axis_index("expert")
    core = index & 1
    half = size // 2
    capacity = min(rows, rows * top // size + 2)
    capacity = -(-capacity // 8) * 8
    index_here = index % half
    owners = index - index_here + (index_here ^ jnp.arange(half, dtype=i32))
    info = jnp.concatenate([jnp.stack([index, core]).astype(i32), owners])

    pieces = gather_latents(latents[0].reshape(local_len, seq_count * latent), size)
    parts = fetch_weights(w_uv, w_out, core, size)
    table = jnp.concatenate([ids[0].astype(f32), gates[0].astype(f32)], axis=2)
    table = jnp.transpose(table, (1, 0, 2)).reshape(rows, 2 * top)
    far_table = flip(table, half, size)

    group = max(1, min(heads, 256 // local_len))
    total_len = size * local_len + mem_latents.shape[1]
    (attended,) = call(
        functools.partial(attend_body, size, local_len, seq_count, latent, heads, group),
        "attend",
        [SMEM, SMEM, VMEM, VMEM] + [VMEM] * size,
        [((rows, heads * latent), bf16)],
        [
            info,
            lengths,
            queries[0].reshape(local_len, seq_count * heads * latent),
            mem_latents[0].reshape(-1, seq_count * latent),
            *pieces,
        ],
        flops=4 * rows * heads * latent * total_len,
        scratch=[pltpu.VMEM((total_len, latent), bf16), pltpu.VMEM((group * local_len, latent), bf16)],
    )
    block = ((capacity, width), bf16)
    wide = half * capacity
    residual, normed, near_mix, *near = call(
        functools.partial(middle_body, len(parts), half, capacity, top, local_len, seq_count, latent),
        "middle",
        [SMEM, SMEM] + [VMEM] * (4 + 2 * len(parts)),
        [((rows, width), f32), ((rows, width), bf16), ((rows, wide), bf16)] + [block] * half,
        [
            info,
            head_order(core, w_uv.shape[0]),
            attended,
            hidden[0].reshape(local_len, seq_count * width),
            norm_gain.reshape(1, width),
            table,
            *[w for part in parts for w in part],
        ],
        flops=2 * rows * width * (heads * w_uv.shape[2] + wide),
    )

    def swap(blocks):
        return [blocks[0]] + [flip(blocks[m], m, size) for m in range(1, half)]

    def experts(blocks):
        return call(
            functools.partial(expert_body, half, capacity),
            "experts",
            [ANY] * 3 + [VMEM] * half,
            [block] * half,
            [w_gate, w_up, w_down, *blocks],
            flops=6 * wide * width * w_gate.shape[2],
            scratch=[pltpu.VMEM(w.shape[1:], bf16) for w in (w_gate, w_up, w_down)]
            + [pltpu.VMEM((wide, width), bf16), pltpu.SemaphoreType.DMA((3,))],
        )

    far_rows = flip(normed, half, size)
    near_in = swap(near)
    far_mix, *far = call(
        functools.partial(far_body, half, capacity, top),
        "far_place",
        [SMEM, VMEM, VMEM],
        [((rows, wide), bf16)] + [block] * half,
        [info, far_table, far_rows],
        flops=2 * rows * width * wide,
    )
    far_in = swap(far)
    near_out = experts(near_in)
    far_out = experts(far_in)
    (far_sum,) = call(
        functools.partial(mix_body, half, capacity),
        "far_mix",
        [VMEM] * (1 + half),
        [((rows, width), bf16)],
        [far_mix, *swap(far_out)],
        flops=2 * rows * width * wide,
        scratch=[pltpu.VMEM((wide, width), bf16)],
    )
    other = flip(far_sum, half, size)
    (out,) = call(
        functools.partial(last_body, half, capacity, local_len, seq_count),
        "last",
        [VMEM] * (3 + half),
        [((local_len, seq_count * width), bf16)],
        [near_mix, residual, other, *swap(near_out)],
        flops=2 * rows * width * wide,
        scratch=[pltpu.VMEM((wide, width), bf16)],
    )
    return out.reshape(1, local_len, seq_count, width)


def solution(mesh):
    return jax.shard_map(
        shards,
        mesh=mesh,
        in_specs=(
            P("dp", "expert", None, None),
            P("dp", "expert", None, None),
            P("dp", "expert", None, None),
            P("dp", None, None, None),
            P("dp", None),
            P("dp", "expert", None, None),
            P("dp", "expert", None, None),
            P(),
            P("dp", None, None),
            P("dp", None),
            P("expert", None, None),
            P("expert", None, None),
            P("expert", None, None),
        ),
        out_specs=P("dp", "expert", None, None),
        check_vma=False,
    )
```

```python
import functools

import jax
import jax.numpy as jnp
from jax import lax
from jax.experimental import pallas as pl
from jax.experimental.pallas import tpu as pltpu
from jax.sharding import PartitionSpec as P


score_scale = 192.0 ** (-0.5)
norm_eps = 1e-06


cuts = 2

bf16, f32, i32 = jnp.bfloat16, jnp.float32, jnp.int32
VMEM = pl.BlockSpec(memory_space=pltpu.VMEM)
SMEM = pl.BlockSpec(memory_space=pltpu.SMEM)
ANY = pl.BlockSpec(memory_space=pl.ANY)


def flip(value, mask, size):
    return lax.ppermute(value, "expert", [(i, i ^ mask) for i in range(size)])


def call(body, in_specs, outs, operands, flops=0, scratch=(), limit=24):
    return pl.pallas_call(
        body,
        in_specs=in_specs,
        out_specs=[VMEM] * len(outs),
        out_shape=[jax.ShapeDtypeStruct(s, d) for s, d in outs],
        scratch_shapes=list(scratch),
        compiler_params=pltpu.CompilerParams(vmem_limit_bytes=limit * 1024 * 1024),
        cost_estimate=pl.CostEstimate(flops=flops, bytes_accessed=0, transcendentals=0),
    )(*operands)


def gather_latents(own, size):
    pieces = {0: own}
    quarter = size // 4
    for mask in (2 * quarter, 3 * quarter, quarter):
        pieces[mask] = flip(own, mask, size)
    step = quarter // 2
    while step:
        for mask in list(pieces):
            pieces[mask ^ step] = flip(pieces[mask], step, size)
        step //= 2
    return [pieces[m] for m in range(size)]


def fetch_weights(w_uv, w_out, core, size):
    dp = lax.axis_size("dp")
    heads = w_uv.shape[0]
    half = heads // 2
    width = w_out.shape[0] // heads
    uv_half = lax.dynamic_slice_in_dim(w_uv, core * half, half, 0)
    out_half = lax.dynamic_slice_in_dim(w_out, core * half * width, half * width, 0)
    parts = [(w_uv, w_out)]
    for turn in range(1, dp):
        source = [((i + turn) % dp, i) for i in range(dp)]
        uv_got = lax.ppermute(uv_half, "dp", source)
        out_got = lax.ppermute(out_half, "dp", source)
        parts.append((uv_got, out_got))
        parts.append((flip(uv_got, 1, size), flip(out_got, 1, size)))
    return parts


def head_order(core, heads):
    dp = lax.axis_size("dp")
    index = lax.axis_index("dp")
    half = heads // 2
    order = [index * heads + h for h in range(heads)]
    for turn in range(1, dp):
        first = ((index + turn) % dp) * heads
        order += [first + core * half + h for h in range(half)]
        order += [first + (1 - core) * half + h for h in range(half)]
    return jnp.stack(order).astype(i32)


def attend_body(size, local_len, seq_count, latent, heads, group, *refs):
    info, lengths, queries, memory = refs[:4]
    pieces = refs[4 : 4 + size]
    out, keys, rows = refs[4 + size :]
    seg_len = size * local_len
    total_len = seg_len + memory.shape[0]
    shift = local_len.bit_length() - 1
    index = info[0]
    at = lax.broadcasted_iota(i32, (local_len, total_len), 1)
    row = lax.broadcasted_iota(i32, (local_len, total_len), 0)
    pos = jnp.left_shift(jnp.bitwise_xor(jnp.right_shift(at, shift), index), shift) + jnp.bitwise_and(
        at, local_len - 1
    )
    pos = jnp.where(at < seg_len, pos, -1)
    causal = pos <= index * local_len + row
    for s in range(seq_count):
        cols = pl.ds(s * latent, latent)
        for m in range(size):
            keys[pl.ds(m * local_len, local_len), :] = pieces[m][:, cols]
        keys[pl.ds(seg_len, memory.shape[0]), :] = memory[:, cols]
        bias = jnp.where(causal & (pos < lengths[0, s]), 0.0, -jnp.inf)
        bias = jnp.concatenate([bias] * group, axis=0)
        for first in range(0, heads, group):
            for h in range(group):
                rows[pl.ds(h * local_len, local_len), :] = queries[
                    :, pl.ds((s * heads + first + h) * latent, latent)
                ]
            scores = lax.dot_general(
                rows[...], keys[...], (((1,), (1,)), ((), ())), preferred_element_type=f32
            )
            scores = scores * score_scale + bias
            top = jnp.max(scores, axis=1, keepdims=True)
            weights = jnp.exp(scores - top)
            total = jnp.sum(weights, axis=1, keepdims=True)
            got = jnp.dot(weights.astype(bf16), keys[...], preferred_element_type=f32) / total
            got = got.astype(bf16)
            for h in range(group):
                out[pl.ds(s * local_len, local_len), pl.ds((first + h) * latent, latent)] = got[
                    h * local_len : (h + 1) * local_len
                ]


def routes(info, table, top, half, capacity):
    rows = table.shape[0]
    table = table[...]
    names, gates = table[:, :top], table[:, top : 2 * top]
    lane = lax.broadcasted_iota(i32, (rows, half), 1)
    named = jnp.zeros((rows, half), f32)
    weight = jnp.zeros((rows, half), f32)
    for m in range(half):
        hit = names == info[2 + m].astype(f32)
        count = jnp.sum(jnp.where(hit, 1.0, 0.0), axis=1, keepdims=True)
        share = jnp.sum(jnp.where(hit, gates, 0.0), axis=1, keepdims=True)
        named = jnp.where(lane == m, count, named)
        weight = jnp.where(lane == m, share, weight)
    r = lax.broadcasted_iota(i32, (rows, rows), 0)
    c = lax.broadcasted_iota(i32, (rows, rows), 1)
    upto = jnp.where(c <= r, 1.0, 0.0).astype(bf16)
    rank = named * jnp.dot(upto, named.astype(bf16), preferred_element_type=f32)
    wide = half * capacity
    col = lax.broadcasted_iota(i32, (half, wide), 1)
    start = lax.broadcasted_iota(i32, (half, wide), 0) * capacity
    inside = (col >= start) & (col < start + capacity)
    spread = jnp.where(inside, 1.0, 0.0).astype(bf16)
    slot = jnp.sum(jnp.where(inside, col - start + 1, 0), axis=0, keepdims=True).astype(f32)
    rank = jnp.dot(rank.astype(bf16), spread, preferred_element_type=f32)
    weight = jnp.dot(weight.astype(bf16), spread, preferred_element_type=f32)
    place = rank == slot
    return jnp.where(place, 1.0, 0.0).astype(bf16), jnp.where(place, weight, 0.0).astype(bf16)


def routes_body(half, capacity, top, info, near_table, far_table, near_place, near_mix, far_place, far_mix):
    near_place[...], near_mix[...] = routes(info, near_table, top, half, capacity)
    far_place[...], far_mix[...] = routes(info, far_table, top, half, capacity)


def place_body(capacity, cuts, placing, *refs):
    across = (((0,), (0,)), ((), ()))
    rows = jnp.concatenate([r[...] for r in refs[:cuts]], axis=1)
    sent = lax.dot_general(placing[...], rows, across, preferred_element_type=f32).astype(bf16)
    for m, block in enumerate(refs[cuts:]):
        block[...] = sent[m * capacity : (m + 1) * capacity]


def norm_body(parts, seq_count, latent, *refs):
    order, attended, hidden, gain = refs[:4]
    maps = refs[4 : 4 + 2 * parts]
    residual = refs[4 + 2 * parts]
    chunks = refs[5 + 2 * parts :]
    width = gain.shape[1]
    acc = jnp.concatenate([hidden[:, s * width : (s + 1) * width] for s in range(seq_count)], axis=0).astype(f32)
    slot = 0
    for part in range(parts):
        uv, proj = maps[2 * part], maps[2 * part + 1]
        values = []
        for h in range(uv.shape[0]):
            at = pl.multiple_of(order[slot] * latent, latent)
            got = jnp.dot(attended[:, pl.ds(at, latent)], uv[h], preferred_element_type=f32)
            values.append(got.astype(bf16))
            slot += 1
        acc = acc + jnp.dot(jnp.concatenate(values, axis=1), proj[...], preferred_element_type=f32)
    residual[...] = acc
    mean_square = jnp.mean(acc * acc, axis=1, keepdims=True)
    scaled = (acc * lax.rsqrt(mean_square + norm_eps) * gain[...].astype(f32)).astype(bf16)
    step = width // len(chunks)
    for c, chunk in enumerate(chunks):
        chunk[...] = scaled[:, c * step : (c + 1) * step]


def expert_body(half, capacity, cuts, *refs):
    gate_hbm, up_hbm, down_hbm = refs[:3]
    count = half * cuts
    taken = refs[3 : 3 + count]
    given = refs[3 + count : 3 + 2 * count]
    gate, up, down, rows, sems = refs[3 + 2 * count :]
    step = rows.shape[1] // cuts
    copies = [
        pltpu.make_async_copy(source.at[0], target, sems.at[i])
        for i, (source, target) in enumerate(((gate_hbm, gate), (up_hbm, up), (down_hbm, down)))
    ]
    for copy in copies:
        copy.start()
    for c in range(cuts):
        for m in range(half):
            rows[pl.ds(m * capacity, capacity), pl.ds(c * step, step)] = taken[c * half + m][...]
    across = (((1,), (1,)), ((), ()))
    copies[0].wait()
    gate_h = lax.dot_general(rows[...], gate[...], across, preferred_element_type=f32)
    copies[1].wait()
    up_h = lax.dot_general(rows[...], up[...], across, preferred_element_type=f32)
    act = (gate_h / (1.0 + jnp.exp(-gate_h)) * up_h).astype(bf16)
    copies[2].wait()
    for c in range(cuts):
        out = jnp.dot(act, down[:, c * step : (c + 1) * step], preferred_element_type=f32).astype(bf16)
        for m in range(half):
            given[c * half + m][...] = out[m * capacity : (m + 1) * capacity]


def mix_body(half, capacity, mixing, *refs):
    taken, out, rows = refs[:half], refs[half], refs[half + 1]
    for m in range(half):
        rows[pl.ds(m * capacity, capacity), :] = taken[m][...]
    out[...] = jnp.dot(mixing[...], rows[...], preferred_element_type=f32).astype(bf16)


def last_body(half, capacity, cuts, local_len, seq_count, mixing, residual, *refs):
    others, taken, out, rows = refs[:cuts], refs[cuts : cuts + half], refs[cuts + half], refs[cuts + half + 1]
    for m in range(half):
        rows[pl.ds(m * capacity, capacity), :] = taken[m][...]
    total = jnp.dot(mixing[...], rows[...], preferred_element_type=f32)
    other = jnp.concatenate([o[...] for o in others], axis=1)
    total = (residual[...] + total + other.astype(f32)).astype(bf16)
    width = total.shape[1]
    for s in range(seq_count):
        out[:, s * width : (s + 1) * width] = total[s * local_len : (s + 1) * local_len]


def layer(
    hidden,
    queries,
    latents,
    mem_latents,
    lengths,
    ids,
    gates,
    norm_gain,
    w_uv,
    w_out,
    w_gate,
    w_up,
    w_down,
):
    local_len, seq_count, width = hidden.shape[1:]
    latent = latents.shape[3]
    heads = queries.shape[3] // latent
    rows = local_len * seq_count
    top = ids.shape[3]
    size = lax.axis_size("expert")
    index = lax.axis_index("expert")
    core = index & 1
    half = size // 2
    capacity = min(rows, rows * top // size + 2)
    capacity = -(-capacity // 8) * 8
    index_here = index % half
    owners = index - index_here + (index_here ^ jnp.arange(half, dtype=i32))
    info = jnp.concatenate([jnp.stack([index, core]).astype(i32), owners])

    parts = fetch_weights(w_uv, w_out, core, size)
    pieces = gather_latents(latents[0].reshape(local_len, seq_count * latent), size)
    table = jnp.concatenate([ids[0].astype(f32), gates[0].astype(f32)], axis=2)
    table = jnp.transpose(table, (1, 0, 2)).reshape(rows, 2 * top)
    far_table = flip(table, half, size)
    wide = half * capacity
    near_placing, near_mix, far_placing, far_mix = call(
        functools.partial(routes_body, half, capacity, top),
        [SMEM, VMEM, VMEM],
        [((rows, wide), bf16)] * 4,
        [info, table, far_table],
        flops=4 * rows * rows * wide,
    )

    group = max(1, min(heads, 256 // local_len))
    total_len = size * local_len + mem_latents.shape[1]
    (attended,) = call(
        functools.partial(attend_body, size, local_len, seq_count, latent, heads, group),
        [SMEM, SMEM, VMEM, VMEM] + [VMEM] * size,
        [((rows, heads * latent), bf16)],
        [
            info,
            lengths,
            queries[0].reshape(local_len, seq_count * heads * latent),
            mem_latents[0].reshape(-1, seq_count * latent),
            *pieces,
        ],
        flops=4 * rows * heads * latent * total_len,
        scratch=[pltpu.VMEM((total_len, latent), bf16), pltpu.VMEM((group * local_len, latent), bf16)],
        limit=16 + total_len * 9 // 1024,
    )
    step = width // cuts
    residual, *normed = call(
        functools.partial(norm_body, len(parts), seq_count, latent),
        [SMEM] + [VMEM] * (3 + 2 * len(parts)),
        [((rows, width), f32)] + [((rows, step), bf16)] * cuts,
        [
            head_order(core, w_uv.shape[0]),
            attended,
            hidden[0].reshape(local_len, seq_count * width),
            norm_gain.reshape(1, width),
            *[w for part in parts for w in part],
        ],
        flops=2 * rows * width * heads * w_uv.shape[2],
    )

    def swap(blocks):
        return [blocks[0]] + [flip(blocks[m], m, size) for m in range(1, half)]

    def place(placing, chunks):
        return call(
            functools.partial(place_body, capacity, len(chunks)),
            [VMEM] * (1 + len(chunks)),
            [((capacity, sum(c.shape[1] for c in chunks)), bf16)] * half,
            [placing, *chunks],
            flops=2 * rows * width * wide,
        )

    def experts(blocks):
        return call(
            functools.partial(expert_body, half, capacity, len(blocks) // half),
            [ANY] * 3 + [VMEM] * len(blocks),
            [(b.shape, bf16) for b in blocks],
            [jnp.swapaxes(w_gate, 1, 2), jnp.swapaxes(w_up, 1, 2), w_down, *blocks],
            flops=6 * wide * width * w_gate.shape[2],
            scratch=[pltpu.VMEM(w_down.shape[1:], bf16)] * 3
            + [pltpu.VMEM((wide, width), bf16), pltpu.SemaphoreType.DMA((3,))],
            limit=32,
        )

    hops = [flip(chunk, half, size) for chunk in normed]
    near_in = swap(place(near_placing, normed))
    far_in = []
    for c in range(cuts):
        far_in += swap(place(far_placing, [hops[c]]))
    near_out = swap(experts(near_in))
    far_out = experts(far_in)
    others = []
    for c in range(cuts):
        (far_sum,) = call(
            functools.partial(mix_body, half, capacity),
            [VMEM] * (1 + half),
            [((rows, step), bf16)],
            [far_mix, *swap(far_out[c * half : (c + 1) * half])],
            flops=2 * rows * step * wide,
            scratch=[pltpu.VMEM((wide, step), bf16)],
        )
        others.append(flip(far_sum, half, size))
    (out,) = call(
        functools.partial(last_body, half, capacity, cuts, local_len, seq_count),
        [VMEM] * (2 + cuts + half),
        [((local_len, seq_count * width), bf16)],
        [near_mix, residual, *others, *near_out],
        flops=2 * rows * width * wide,
        scratch=[pltpu.VMEM((wide, width), bf16)],
    )
    return out.reshape(1, local_len, seq_count, width)


def solution(mesh):
    return spread(mesh)


def spread(mesh):
    return jax.shard_map(
        layer,
        mesh=mesh,
        in_specs=(
            P("dp", "expert", None, None),
            P("dp", "expert", None, None),
            P("dp", "expert", None, None),
            P("dp", None, None, None),
            P("dp", None),
            P("dp", "expert", None, None),
            P("dp", "expert", None, None),
            P(),
            P("dp", None, None),
            P("dp", None),
            P("expert", None, None),
            P("expert", None, None),
            P("expert", None, None),
        ),
        out_specs=P("dp", "expert", None, None),
        check_vma=False,
    )
```

```python
import functools

import jax
import jax.numpy as jnp
from jax import lax
from jax.experimental import pallas as pl
from jax.experimental.pallas import tpu as pltpu
from jax.sharding import PartitionSpec as P


score_scale = 192.0 ** (-0.5)
norm_eps = 1e-06


cuts = 2

bf16, f32, i32 = jnp.bfloat16, jnp.float32, jnp.int32
VMEM = pl.BlockSpec(memory_space=pltpu.VMEM)
SMEM = pl.BlockSpec(memory_space=pltpu.SMEM)
ANY = pl.BlockSpec(memory_space=pl.ANY)


def flip(value, mask, size):
    return lax.ppermute(value, "expert", [(i, i ^ mask) for i in range(size)])


def call(body, in_specs, outs, operands, flops=0, scratch=(), limit=24):
    return pl.pallas_call(
        body,
        in_specs=in_specs,
        out_specs=[VMEM] * len(outs),
        out_shape=[jax.ShapeDtypeStruct(s, d) for s, d in outs],
        scratch_shapes=list(scratch),
        compiler_params=pltpu.CompilerParams(vmem_limit_bytes=limit * 1024 * 1024),
        cost_estimate=pl.CostEstimate(flops=flops, bytes_accessed=0, transcendentals=0),
    )(*operands)


def gather_latents(own, size, beside):
    pieces = {0: own}
    quarter = size // 4
    for mask in (2 * quarter, 3 * quarter, quarter):
        pieces[mask] = flip(own, mask, size)
    pieces[3 * quarter], beside = lax.optimization_barrier((pieces[3 * quarter], beside))
    step = quarter // 2
    while step:
        for mask in list(pieces):
            pieces[mask ^ step] = flip(pieces[mask], step, size)
        step //= 2
    return [pieces[m] for m in range(size)], beside


def fetch_weights(w_uv, w_out, core, size):
    dp = lax.axis_size("dp")
    heads = w_uv.shape[0]
    half = heads // 2
    width = w_out.shape[0] // heads
    uv_half = lax.dynamic_slice_in_dim(w_uv, core * half, half, 0)
    out_half = lax.dynamic_slice_in_dim(w_out, core * half * width, half * width, 0)
    parts = [(w_uv, w_out)]
    for turn in range(1, dp):
        source = [((i + turn) % dp, i) for i in range(dp)]
        uv_got = lax.ppermute(uv_half, "dp", source)
        out_got = lax.ppermute(out_half, "dp", source)
        parts.append((uv_got, out_got))
        parts.append((flip(uv_got, 1, size), flip(out_got, 1, size)))
    return parts


def head_order(core, heads):
    dp = lax.axis_size("dp")
    index = lax.axis_index("dp")
    half = heads // 2
    order = [index * heads + h for h in range(heads)]
    for turn in range(1, dp):
        first = ((index + turn) % dp) * heads
        order += [first + core * half + h for h in range(half)]
        order += [first + (1 - core) * half + h for h in range(half)]
    return jnp.stack(order).astype(i32)


def attend_body(size, local_len, seq_count, latent, heads, group, *refs):
    info, lengths, queries, memory = refs[:4]
    pieces = refs[4 : 4 + size]
    out, keys, rows = refs[4 + size :]
    seg_len = size * local_len
    total_len = seg_len + memory.shape[0]
    shift = local_len.bit_length() - 1
    index = info[0]
    at = lax.broadcasted_iota(i32, (local_len, total_len), 1)
    row = lax.broadcasted_iota(i32, (local_len, total_len), 0)
    pos = jnp.left_shift(jnp.bitwise_xor(jnp.right_shift(at, shift), index), shift) + jnp.bitwise_and(
        at, local_len - 1
    )
    pos = jnp.where(at < seg_len, pos, -1)
    causal = pos <= index * local_len + row
    for s in range(seq_count):
        cols = pl.ds(s * latent, latent)
        for m in range(size):
            keys[pl.ds(m * local_len, local_len), :] = pieces[m][:, cols]
        keys[pl.ds(seg_len, memory.shape[0]), :] = memory[:, cols]
        bias = jnp.where(causal & (pos < lengths[0, s]), 0.0, -jnp.inf)
        bias = jnp.concatenate([bias] * group, axis=0)
        for first in range(0, heads, group):
            for h in range(group):
                rows[pl.ds(h * local_len, local_len), :] = queries[
                    :, pl.ds((s * heads + first + h) * latent, latent)
                ]
            scores = lax.dot_general(
                rows[...], keys[...], (((1,), (1,)), ((), ())), preferred_element_type=f32
            )
            scores = scores * score_scale + bias
            top = jnp.max(scores, axis=1, keepdims=True)
            weights = jnp.exp(scores - top)
            total = jnp.sum(weights, axis=1, keepdims=True)
            got = jnp.dot(weights.astype(bf16), keys[...], preferred_element_type=f32) / total
            got = got.astype(bf16)
            for h in range(group):
                out[pl.ds(s * local_len, local_len), pl.ds((first + h) * latent, latent)] = got[
                    h * local_len : (h + 1) * local_len
                ]


def pack(block, value, capacity):
    lanes = block.shape[1]
    for j in range(value.shape[1] // lanes):
        block[j * capacity : (j + 1) * capacity, :] = value[:capacity, j * lanes : (j + 1) * lanes]


def unpack(rows, at, column, block, capacity):
    lanes = block.shape[1]
    for j in range(block.shape[0] // capacity):
        first = column + j * lanes
        rows[at : at + capacity, first : first + lanes] = block[j * capacity : (j + 1) * capacity, :]


def routes(info, table, top, half, pitch):
    rows = table.shape[0]
    table = table[...]
    names, gates = table[:, :top], table[:, top : 2 * top]
    lane = lax.broadcasted_iota(i32, (rows, half), 1)
    named = jnp.zeros((rows, half), f32)
    weight = jnp.zeros((rows, half), f32)
    for m in range(half):
        hit = names == info[2 + m].astype(f32)
        count = jnp.sum(jnp.where(hit, 1.0, 0.0), axis=1, keepdims=True)
        share = jnp.sum(jnp.where(hit, gates, 0.0), axis=1, keepdims=True)
        named = jnp.where(lane == m, count, named)
        weight = jnp.where(lane == m, share, weight)
    r = lax.broadcasted_iota(i32, (rows, rows), 0)
    c = lax.broadcasted_iota(i32, (rows, rows), 1)
    upto = jnp.where(c <= r, 1.0, 0.0).astype(bf16)
    rank = named * jnp.dot(upto, named.astype(bf16), preferred_element_type=f32)
    wide = half * pitch
    col = lax.broadcasted_iota(i32, (half, wide), 1)
    start = lax.broadcasted_iota(i32, (half, wide), 0) * pitch
    inside = (col >= start) & (col < start + pitch)
    spread = jnp.where(inside, 1.0, 0.0).astype(bf16)
    slot = jnp.sum(jnp.where(inside, col - start + 1, 0), axis=0, keepdims=True).astype(f32)
    rank = jnp.dot(rank.astype(bf16), spread, preferred_element_type=f32)
    weight = jnp.dot(weight.astype(bf16), spread, preferred_element_type=f32)
    place = rank == slot
    return jnp.where(place, 1.0, 0.0).astype(bf16), jnp.where(place, weight, 0.0).astype(bf16)


def routes_body(half, quarter, pitch, top, info, *refs):
    count = len(refs) // 3
    for i, here in enumerate((half, quarter, half)):
        refs[count + 2 * i][...], refs[count + 2 * i + 1][...] = routes(info, refs[i], top, here, pitch)


def place_body(pitch, capacity, cuts, placing, *refs):
    across = (((0,), (0,)), ((), ()))
    rows = jnp.concatenate([r[...] for r in refs[:cuts]], axis=1)
    sent = lax.dot_general(placing[...], rows, across, preferred_element_type=f32).astype(bf16)
    for m, block in enumerate(refs[cuts:]):
        pack(block, sent[m * pitch : (m + 1) * pitch], capacity)


def norm_body(parts, seq_count, latent, *refs):
    order, attended, hidden, gain = refs[:4]
    maps = refs[4 : 4 + 2 * parts]
    residual = refs[4 + 2 * parts]
    chunks = refs[5 + 2 * parts :]
    width = gain.shape[1]
    acc = jnp.concatenate([hidden[:, s * width : (s + 1) * width] for s in range(seq_count)], axis=0).astype(f32)
    slot = 0
    for part in range(parts):
        uv, proj = maps[2 * part], maps[2 * part + 1]
        values = []
        for h in range(uv.shape[0]):
            at = pl.multiple_of(order[slot] * latent, latent)
            got = jnp.dot(attended[:, pl.ds(at, latent)], uv[h], preferred_element_type=f32)
            values.append(got.astype(bf16))
            slot += 1
        acc = acc + jnp.dot(jnp.concatenate(values, axis=1), proj[...], preferred_element_type=f32)
    residual[...] = acc
    mean_square = jnp.mean(acc * acc, axis=1, keepdims=True)
    scaled = (acc * lax.rsqrt(mean_square + norm_eps) * gain[...].astype(f32)).astype(bf16)
    step = width // len(chunks)
    for c, chunk in enumerate(chunks):
        chunk[...] = scaled[:, c * step : (c + 1) * step]


def expert_body(count, pitch, capacity, cuts, *refs):
    gate_hbm, up_hbm, down_hbm = refs[:3]
    taken = refs[3 : 3 + count * cuts]
    given = refs[3 + count * cuts : -5]
    gate, up, down, rows, sems = refs[-5:]
    step = rows.shape[1] // cuts
    copies = [
        pltpu.make_async_copy(source.at[0], target, sems.at[i])
        for i, (source, target) in enumerate(((gate_hbm, gate), (up_hbm, up), (down_hbm, down)))
    ]
    for copy in copies:
        copy.start()
    for c in range(cuts):
        for m in range(count):
            unpack(rows, m * pitch, c * step, taken[c * count + m], capacity)
    across = (((1,), (1,)), ((), ()))
    copies[0].wait()
    gate_h = lax.dot_general(rows[...], gate[...], across, preferred_element_type=f32)
    copies[1].wait()
    up_h = lax.dot_general(rows[...], up[...], across, preferred_element_type=f32)
    act = (gate_h / (1.0 + jnp.exp(-gate_h)) * up_h).astype(bf16)
    copies[2].wait()
    for c in range(cuts):
        out = jnp.dot(act, down[:, c * step : (c + 1) * step], preferred_element_type=f32).astype(bf16)
        for m in range(count):
            pack(given[c * count + m], out[m * pitch : (m + 1) * pitch], capacity)


def mix_body(half, pitch, capacity, mixing, *refs):
    taken, out, rows = refs[:half], refs[half], refs[half + 1]
    rows[...] = jnp.zeros(rows.shape, bf16)
    for m in range(half):
        unpack(rows, m * pitch, 0, taken[m], capacity)
    out[...] = jnp.dot(mixing[...], rows[...], preferred_element_type=f32).astype(bf16)


def near_mix_body(half, pitch, capacity, mixing, residual, *refs):
    taken, total, rows = refs[:half], refs[half], refs[half + 1]
    rows[...] = jnp.zeros(rows.shape, bf16)
    for m in range(half):
        unpack(rows, m * pitch, 0, taken[m], capacity)
    total[...] = residual[...] + jnp.dot(mixing[...], rows[...], preferred_element_type=f32)


def last_body(local_len, seq_count, total, *refs):
    others, out = refs[:-1], refs[-1]
    other = jnp.concatenate([o[...] for o in others], axis=1).astype(f32)
    done = (total[...] + other).astype(bf16)
    width = done.shape[1]
    for s in range(seq_count):
        out[:, s * width : (s + 1) * width] = done[s * local_len : (s + 1) * local_len]


def layer(
    hidden,
    queries,
    latents,
    mem_latents,
    lengths,
    ids,
    gates,
    norm_gain,
    w_uv,
    w_out,
    w_gate,
    w_up,
    w_down,
):
    local_len, seq_count, width = hidden.shape[1:]
    latent = latents.shape[3]
    heads = queries.shape[3] // latent
    rows = local_len * seq_count
    top = ids.shape[3]
    size = lax.axis_size("expert")
    index = lax.axis_index("expert")
    core = index & 1
    half = size // 2
    capacity = min(rows, rows * top // size + 2)
    pitch = -(-capacity // 8) * 8
    lanes = 128
    index_here = index % half
    owners = index - index_here + (index_here ^ jnp.arange(half, dtype=i32))
    info = jnp.concatenate([jnp.stack([index, core]).astype(i32), owners])

    quarter = half // 2
    parts = fetch_weights(w_uv, w_out, core, size)
    beside = (
        queries[0].reshape(local_len, seq_count * heads * latent),
        hidden[0].reshape(local_len, seq_count * width),
        mem_latents[0].reshape(-1, seq_count * latent),
    )
    own_latents = latents[0].reshape(local_len, seq_count * latent)
    pieces, (query_rows, hidden_rows, memory) = gather_latents(own_latents, size, beside)
    table = jnp.concatenate([ids[0].astype(f32), gates[0].astype(f32)], axis=2)
    table = jnp.transpose(table, (1, 0, 2)).reshape(rows, 2 * top)
    far_table = flip(table, half, size)
    side_table = flip(table, quarter, size)
    wide = half * pitch
    short = quarter * pitch
    near_placing, near_mix, side_placing, _, far_placing, far_mix = call(
        functools.partial(routes_body, half, quarter, pitch, top),
        [SMEM] + [VMEM] * 3,
        [((rows, wide), bf16)] * 2 + [((rows, short), bf16)] * 2 + [((rows, wide), bf16)] * 2,
        [info, table, side_table, far_table],
        flops=4 * rows * rows * wide,
    )

    group = max(1, min(heads, 256 // local_len))
    total_len = size * local_len + mem_latents.shape[1]
    (attended,) = call(
        functools.partial(attend_body, size, local_len, seq_count, latent, heads, group),
        [SMEM, SMEM, VMEM, VMEM] + [VMEM] * size,
        [((rows, heads * latent), bf16)],
        [
            info,
            lengths,
            query_rows,
            memory,
            *pieces,
        ],
        flops=4 * rows * heads * latent * total_len,
        scratch=[pltpu.VMEM((total_len, latent), bf16), pltpu.VMEM((group * local_len, latent), bf16)],
        limit=16 + total_len * 9 // 1024,
    )
    step = width // cuts
    residual, *normed = call(
        functools.partial(norm_body, len(parts), seq_count, latent),
        [SMEM] + [VMEM] * (3 + 2 * len(parts)),
        [((rows, width), f32)] + [((rows, step), bf16)] * cuts,
        [
            head_order(core, w_uv.shape[0]),
            attended,
            hidden_rows,
            norm_gain.reshape(1, width),
            *[w for part in parts for w in part],
        ],
        flops=2 * rows * width * heads * w_uv.shape[2],
    )

    def swap(blocks):
        return [blocks[0]] + [flip(blocks[m], m, size) for m in range(1, len(blocks))]

    def place(placing, chunks):
        count = placing.shape[1] // pitch
        sent = (capacity * sum(c.shape[1] for c in chunks) // lanes, lanes)
        return call(
            functools.partial(place_body, pitch, capacity, len(chunks)),
            [VMEM] * (1 + len(chunks)),
            [(sent, bf16)] * count,
            [placing, *chunks],
            flops=2 * rows * width * wide,
        )

    def experts(blocks, column_cuts):
        count = len(blocks) // column_cuts
        return call(
            functools.partial(expert_body, count, pitch, capacity, column_cuts),
            [ANY] * 3 + [VMEM] * len(blocks),
            [(b.shape, bf16) for b in blocks],
            [jnp.swapaxes(w_gate, 1, 2), jnp.swapaxes(w_up, 1, 2), w_down, *blocks],
            flops=6 * wide * width * w_gate.shape[2],
            scratch=[pltpu.VMEM(w_down.shape[1:], bf16)] * 3
            + [pltpu.VMEM((count * pitch, width), bf16), pltpu.SemaphoreType.DMA((3,))],
            limit=32,
        )

    hops = [flip(normed[c], half, size) for c in range(cuts)]
    sides = [flip(normed[c], quarter, size) for c in range(cuts)]
    near_in = swap(place(near_placing[:, :short], normed))
    near_in += swap(place(side_placing, sides))
    far_in = []
    for c in range(cuts):
        far_in += swap(place(far_placing, [hops[c]]))
    near_out = experts(near_in, 1)
    near_back = [near_out[0]] + [flip(near_out[m], m, size) for m in range(1, quarter)]
    near_back += [flip(near_out[m], m, size) for m in range(quarter, half)]
    far_out = experts(far_in, cuts)
    others = []
    for c in range(cuts):
        (far_sum,) = call(
            functools.partial(mix_body, half, pitch, capacity),
            [VMEM] * (1 + half),
            [((rows, step), bf16)],
            [far_mix, *swap(far_out[c * half : (c + 1) * half])],
            flops=2 * rows * step * wide,
            scratch=[pltpu.VMEM((wide, step), bf16)],
        )
        others.append(flip(far_sum, half, size))
    (total,) = call(
        functools.partial(near_mix_body, half, pitch, capacity),
        [VMEM] * (2 + half),
        [((rows, width), f32)],
        [near_mix, residual, *near_back],
        flops=2 * rows * width * wide,
        scratch=[pltpu.VMEM((wide, width), bf16)],
    )
    (out,) = call(
        functools.partial(last_body, local_len, seq_count),
        [VMEM] * (1 + cuts),
        [((local_len, seq_count * width), bf16)],
        [total, *others],
        flops=8 * rows * width,
    )
    return out.reshape(1, local_len, seq_count, width)


def solution(mesh):
    return spread(mesh)


def spread(mesh):
    return jax.shard_map(
        layer,
        mesh=mesh,
        in_specs=(
            P("dp", "expert", None, None),
            P("dp", "expert", None, None),
            P("dp", "expert", None, None),
            P("dp", None, None, None),
            P("dp", None),
            P("dp", "expert", None, None),
            P("dp", "expert", None, None),
            P(),
            P("dp", None, None),
            P("dp", None),
            P("expert", None, None),
            P("expert", None, None),
            P("expert", None, None),
        ),
        out_specs=P("dp", "expert", None, None),
        check_vma=False,
    )
```

```python
import functools

import jax
import jax.numpy as jnp
from jax import lax
from jax.experimental import pallas as pl
from jax.experimental.pallas import tpu as pltpu
from jax.sharding import PartitionSpec as P


score_scale = 192.0 ** (-0.5)
norm_eps = 1e-06


cuts = 2

bf16, f32, i32 = jnp.bfloat16, jnp.float32, jnp.int32
VMEM = pl.BlockSpec(memory_space=pltpu.VMEM)
SMEM = pl.BlockSpec(memory_space=pltpu.SMEM)
ANY = pl.BlockSpec(memory_space=pl.ANY)


def flip(value, mask, size):
    return lax.ppermute(value, "expert", [(i, i ^ mask) for i in range(size)])


def call(body, in_specs, outs, operands, flops=0, scratch=(), limit=24):
    return pl.pallas_call(
        body,
        in_specs=in_specs,
        out_specs=[VMEM] * len(outs),
        out_shape=[jax.ShapeDtypeStruct(s, d) for s, d in outs],
        scratch_shapes=list(scratch),
        compiler_params=pltpu.CompilerParams(vmem_limit_bytes=limit * 1024 * 1024),
        cost_estimate=pl.CostEstimate(flops=flops, bytes_accessed=0, transcendentals=0),
    )(*operands)


def gather_latents(own, size, beside):
    pieces = {0: own}
    quarter = size // 4
    for mask in (2 * quarter, 3 * quarter, quarter):
        pieces[mask] = flip(own, mask, size)
    pieces[3 * quarter], beside = lax.optimization_barrier((pieces[3 * quarter], beside))
    step = quarter // 2
    while step:
        for mask in list(pieces):
            pieces[mask ^ step] = flip(pieces[mask], step, size)
        step //= 2
    return [pieces[m] for m in range(size)], beside


def fetch_weights(w_uv, w_out, core, size):
    dp = lax.axis_size("dp")
    heads = w_uv.shape[0]
    half = heads // 2
    width = w_out.shape[0] // heads
    uv_half = lax.dynamic_slice_in_dim(w_uv, core * half, half, 0)
    out_half = lax.dynamic_slice_in_dim(w_out, core * half * width, half * width, 0)
    parts = [(w_uv, w_out)]
    for turn in range(1, dp):
        source = [((i + turn) % dp, i) for i in range(dp)]
        uv_got = lax.ppermute(uv_half, "dp", source)
        out_got = lax.ppermute(out_half, "dp", source)
        parts.append((uv_got, out_got))
        parts.append((flip(uv_got, 1, size), flip(out_got, 1, size)))
    return parts


def head_order(core, heads):
    dp = lax.axis_size("dp")
    index = lax.axis_index("dp")
    half = heads // 2
    order = [index * heads + h for h in range(heads)]
    for turn in range(1, dp):
        first = ((index + turn) % dp) * heads
        order += [first + core * half + h for h in range(half)]
        order += [first + (1 - core) * half + h for h in range(half)]
    return jnp.stack(order).astype(i32)


def attend_body(size, local_len, seq_count, latent, heads, group, *refs):
    info, lengths, queries, memory = refs[:4]
    pieces = refs[4 : 4 + size]
    out, keys, rows = refs[4 + size :]
    seg_len = size * local_len
    total_len = seg_len + memory.shape[0]
    shift = local_len.bit_length() - 1
    index = info[0]
    at = lax.broadcasted_iota(i32, (local_len, total_len), 1)
    row = lax.broadcasted_iota(i32, (local_len, total_len), 0)
    pos = jnp.left_shift(jnp.bitwise_xor(jnp.right_shift(at, shift), index), shift) + jnp.bitwise_and(
        at, local_len - 1
    )
    pos = jnp.where(at < seg_len, pos, -1)
    causal = pos <= index * local_len + row
    for s in range(seq_count):
        cols = pl.ds(s * latent, latent)
        for m in range(size):
            keys[pl.ds(m * local_len, local_len), :] = pieces[m][:, cols]
        keys[pl.ds(seg_len, memory.shape[0]), :] = memory[:, cols]
        bias = jnp.where(causal & (pos < lengths[0, s]), 0.0, -jnp.inf)
        bias = jnp.concatenate([bias] * group, axis=0)
        for first in range(0, heads, group):
            for h in range(group):
                rows[pl.ds(h * local_len, local_len), :] = queries[
                    :, pl.ds((s * heads + first + h) * latent, latent)
                ]
            scores = lax.dot_general(
                rows[...], keys[...], (((1,), (1,)), ((), ())), preferred_element_type=f32
            )
            scores = scores * score_scale + bias
            top = jnp.max(scores, axis=1, keepdims=True)
            weights = jnp.exp(scores - top)
            total = jnp.sum(weights, axis=1, keepdims=True)
            got = jnp.dot(weights.astype(bf16), keys[...], preferred_element_type=f32) / total
            got = got.astype(bf16)
            for h in range(group):
                out[pl.ds(s * local_len, local_len), pl.ds((first + h) * latent, latent)] = got[
                    h * local_len : (h + 1) * local_len
                ]


def pack(block, value, capacity):
    lanes = block.shape[1]
    for j in range(value.shape[1] // lanes):
        block[j * capacity : (j + 1) * capacity, :] = value[:capacity, j * lanes : (j + 1) * lanes]


def unpack(rows, at, column, block, capacity):
    lanes = block.shape[1]
    for j in range(block.shape[0] // capacity):
        first = column + j * lanes
        rows[at : at + capacity, first : first + lanes] = block[j * capacity : (j + 1) * capacity, :]


def routes(info, table, top, half, pitch):
    rows = table.shape[0]
    table = table[...]
    names, gates = table[:, :top], table[:, top : 2 * top]
    lane = lax.broadcasted_iota(i32, (rows, half), 1)
    named = jnp.zeros((rows, half), f32)
    weight = jnp.zeros((rows, half), f32)
    for m in range(half):
        hit = names == info[2 + m].astype(f32)
        count = jnp.sum(jnp.where(hit, 1.0, 0.0), axis=1, keepdims=True)
        share = jnp.sum(jnp.where(hit, gates, 0.0), axis=1, keepdims=True)
        named = jnp.where(lane == m, count, named)
        weight = jnp.where(lane == m, share, weight)
    r = lax.broadcasted_iota(i32, (rows, rows), 0)
    c = lax.broadcasted_iota(i32, (rows, rows), 1)
    upto = jnp.where(c <= r, 1.0, 0.0).astype(bf16)
    rank = named * jnp.dot(upto, named.astype(bf16), preferred_element_type=f32)
    wide = half * pitch
    col = lax.broadcasted_iota(i32, (half, wide), 1)
    start = lax.broadcasted_iota(i32, (half, wide), 0) * pitch
    inside = (col >= start) & (col < start + pitch)
    spread = jnp.where(inside, 1.0, 0.0).astype(bf16)
    slot = jnp.sum(jnp.where(inside, col - start + 1, 0), axis=0, keepdims=True).astype(f32)
    rank = jnp.dot(rank.astype(bf16), spread, preferred_element_type=f32)
    weight = jnp.dot(weight.astype(bf16), spread, preferred_element_type=f32)
    place = rank == slot
    return jnp.where(place, 1.0, 0.0).astype(bf16), jnp.where(place, weight, 0.0).astype(bf16)


def routes_body(half, quarter, pitch, top, info, own, side, far, own_place, near_mix, side_place, far_place, far_mix):
    placing, near_mix[...] = routes(info, own, top, half, pitch)
    own_place[...] = placing[:, : quarter * pitch]
    side_place[...], _ = routes(info, side, top, quarter, pitch)
    far_place[...], far_mix[...] = routes(info, far, top, half, pitch)


def place_body(pitch, capacity, cuts, placing, *refs):
    across = (((0,), (0,)), ((), ()))
    rows = jnp.concatenate([r[...] for r in refs[:cuts]], axis=1)
    sent = lax.dot_general(placing[...], rows, across, preferred_element_type=f32).astype(bf16)
    for m, block in enumerate(refs[cuts:]):
        pack(block, sent[m * pitch : (m + 1) * pitch], capacity)


def norm_body(parts, seq_count, latent, *refs):
    order, attended, hidden, gain = refs[:4]
    maps = refs[4 : 4 + 2 * parts]
    residual = refs[4 + 2 * parts]
    chunks = refs[5 + 2 * parts :]
    width = gain.shape[1]
    acc = jnp.concatenate([hidden[:, s * width : (s + 1) * width] for s in range(seq_count)], axis=0).astype(f32)
    slot = 0
    for part in range(parts):
        uv, proj = maps[2 * part], maps[2 * part + 1]
        values = []
        for h in range(uv.shape[0]):
            at = pl.multiple_of(order[slot] * latent, latent)
            got = jnp.dot(attended[:, pl.ds(at, latent)], uv[h], preferred_element_type=f32)
            values.append(got.astype(bf16))
            slot += 1
        acc = acc + jnp.dot(jnp.concatenate(values, axis=1), proj[...], preferred_element_type=f32)
    residual[...] = acc
    mean_square = jnp.mean(acc * acc, axis=1, keepdims=True)
    scaled = (acc * lax.rsqrt(mean_square + norm_eps) * gain[...].astype(f32)).astype(bf16)
    step = width // len(chunks)
    for c, chunk in enumerate(chunks):
        chunk[...] = scaled[:, c * step : (c + 1) * step]


def expert_body(count, pitch, capacity, cuts, gate, up, down, *refs):
    taken = refs[: count * cuts]
    given = refs[count * cuts : -1]
    rows = refs[-1]
    step = rows.shape[1] // cuts
    for c in range(cuts):
        for m in range(count):
            unpack(rows, m * pitch, c * step, taken[c * count + m], capacity)
    across = (((1,), (1,)), ((), ()))
    gate_h = lax.dot_general(rows[...], gate[0], across, preferred_element_type=f32)
    up_h = lax.dot_general(rows[...], up[0], across, preferred_element_type=f32)
    act = (gate_h / (1.0 + jnp.exp(-gate_h)) * up_h).astype(bf16)
    for c in range(cuts):
        out = jnp.dot(act, down[0, :, c * step : (c + 1) * step], preferred_element_type=f32).astype(bf16)
        for m in range(count):
            pack(given[c * count + m], out[m * pitch : (m + 1) * pitch], capacity)


def mix_body(half, pitch, capacity, mixing, *refs):
    taken, out, rows = refs[:half], refs[half], refs[half + 1]
    rows[...] = jnp.zeros(rows.shape, bf16)
    for m in range(half):
        unpack(rows, m * pitch, 0, taken[m], capacity)
    out[...] = jnp.dot(mixing[...], rows[...], preferred_element_type=f32).astype(bf16)


def near_mix_body(half, pitch, capacity, mixing, residual, *refs):
    taken, total, rows = refs[:half], refs[half], refs[half + 1]
    rows[...] = jnp.zeros(rows.shape, bf16)
    for m in range(half):
        unpack(rows, m * pitch, 0, taken[m], capacity)
    total[...] = residual[...] + jnp.dot(mixing[...], rows[...], preferred_element_type=f32)


def last_body(local_len, seq_count, total, *refs):
    others, out = refs[:-1], refs[-1]
    other = jnp.concatenate([o[...] for o in others], axis=1).astype(f32)
    done = (total[...] + other).astype(bf16)
    width = done.shape[1]
    for s in range(seq_count):
        out[:, s * width : (s + 1) * width] = done[s * local_len : (s + 1) * local_len]


def layer(
    hidden,
    queries,
    latents,
    mem_latents,
    lengths,
    ids,
    gates,
    norm_gain,
    w_uv,
    w_out,
    w_gate,
    w_up,
    w_down,
):
    local_len, seq_count, width = hidden.shape[1:]
    latent = latents.shape[3]
    heads = queries.shape[3] // latent
    rows = local_len * seq_count
    top = ids.shape[3]
    size = lax.axis_size("expert")
    index = lax.axis_index("expert")
    core = index & 1
    half = size // 2
    capacity = min(rows, rows * top // size + 2)
    pitch = -(-capacity // 8) * 8
    lanes = 128
    index_here = index % half
    owners = index - index_here + (index_here ^ jnp.arange(half, dtype=i32))
    info = jnp.concatenate([jnp.stack([index, core]).astype(i32), owners])

    quarter = half // 2
    parts = fetch_weights(w_uv, w_out, core, size)
    beside = (
        queries[0].reshape(local_len, seq_count * heads * latent),
        hidden[0].reshape(local_len, seq_count * width),
        mem_latents[0].reshape(-1, seq_count * latent),
    )
    own_latents = latents[0].reshape(local_len, seq_count * latent)
    pieces, (query_rows, hidden_rows, memory) = gather_latents(own_latents, size, beside)
    table = jnp.concatenate([ids[0].astype(f32), gates[0].astype(f32)], axis=2)
    table = jnp.transpose(table, (1, 0, 2)).reshape(rows, 2 * top)
    far_table = flip(table, half, size)
    side_table = flip(table, quarter, size)
    wide = half * pitch
    short = quarter * pitch
    own_placing, near_mix, side_placing, far_placing, far_mix = call(
        functools.partial(routes_body, half, quarter, pitch, top),
        [SMEM] + [VMEM] * 3,
        [((rows, short), bf16), ((rows, wide), bf16), ((rows, short), bf16)] + [((rows, wide), bf16)] * 2,
        [info, table, side_table, far_table],
        flops=4 * rows * rows * wide,
    )

    group = max(1, min(heads, 256 // local_len))
    total_len = size * local_len + mem_latents.shape[1]
    (attended,) = call(
        functools.partial(attend_body, size, local_len, seq_count, latent, heads, group),
        [SMEM, SMEM, VMEM, VMEM] + [VMEM] * size,
        [((rows, heads * latent), bf16)],
        [
            info,
            lengths,
            query_rows,
            memory,
            *pieces,
        ],
        flops=4 * rows * heads * latent * total_len,
        scratch=[pltpu.VMEM((total_len, latent), bf16), pltpu.VMEM((group * local_len, latent), bf16)],
        limit=16 + total_len * 9 // 1024,
    )
    step = width // cuts
    residual, *normed = call(
        functools.partial(norm_body, len(parts), seq_count, latent),
        [SMEM] + [VMEM] * (3 + 2 * len(parts)),
        [((rows, width), f32)] + [((rows, step), bf16)] * cuts,
        [
            head_order(core, w_uv.shape[0]),
            attended,
            hidden_rows,
            norm_gain.reshape(1, width),
            *[w for part in parts for w in part],
        ],
        flops=2 * rows * width * heads * w_uv.shape[2],
    )

    def swap(blocks):
        return [blocks[0]] + [flip(blocks[m], m, size) for m in range(1, len(blocks))]

    def place(placing, chunks):
        count = placing.shape[1] // pitch
        sent = (capacity * sum(c.shape[1] for c in chunks) // lanes, lanes)
        return call(
            functools.partial(place_body, pitch, capacity, len(chunks)),
            [VMEM] * (1 + len(chunks)),
            [(sent, bf16)] * count,
            [placing, *chunks],
            flops=2 * rows * width * wide,
        )

    def experts(blocks, column_cuts):
        count = len(blocks) // column_cuts
        return call(
            functools.partial(expert_body, count, pitch, capacity, column_cuts),
            [VMEM] * (3 + len(blocks)),
            [(b.shape, bf16) for b in blocks],
            [jnp.swapaxes(w_gate, 1, 2), jnp.swapaxes(w_up, 1, 2), w_down, *blocks],
            flops=6 * wide * width * w_gate.shape[2],
            scratch=[pltpu.VMEM((count * pitch, width), bf16)],
        )

    hops = [flip(normed[c], half, size) for c in range(cuts)]
    sides = [flip(normed[c], quarter, size) for c in range(cuts)]
    own_in = swap(place(own_placing, normed))
    side_in = swap(place(side_placing, sides))
    far_in = [swap(place(far_placing, [hops[c]])) for c in range(cuts)]
    own_out = experts(own_in, 1)
    side_out = experts(side_in, 1)
    near_back = [own_out[0]] + [flip(own_out[m], m, size) for m in range(1, quarter)]
    near_back += [flip(side_out[m], m + quarter, size) for m in range(quarter)]
    far_out = experts([b for chunk in far_in for b in chunk], cuts)
    others = []
    for c in range(cuts):
        sent = far_out[c * half : (c + 1) * half]
        got = [sent[0]] + [flip(sent[m], m, size) for m in range(1, quarter)]
        got += [flip(sent[m], m, size) for m in range(quarter, half)]
        (far_sum,) = call(
            functools.partial(mix_body, half, pitch, capacity),
            [VMEM] * (1 + half),
            [((rows, step), bf16)],
            [far_mix, *got],
            flops=2 * rows * step * wide,
            scratch=[pltpu.VMEM((wide, step), bf16)],
        )
        others.append(flip(far_sum, half, size))
    (total,) = call(
        functools.partial(near_mix_body, half, pitch, capacity),
        [VMEM] * (2 + half),
        [((rows, width), f32)],
        [near_mix, residual, *near_back],
        flops=2 * rows * width * wide,
        scratch=[pltpu.VMEM((wide, width), bf16)],
    )
    (out,) = call(
        functools.partial(last_body, local_len, seq_count),
        [VMEM] * (1 + cuts),
        [((local_len, seq_count * width), bf16)],
        [total, *others],
        flops=8 * rows * width,
    )
    return out.reshape(1, local_len, seq_count, width)


def solution(mesh):
    return spread(mesh)


def spread(mesh):
    return jax.shard_map(
        layer,
        mesh=mesh,
        in_specs=(
            P("dp", "expert", None, None),
            P("dp", "expert", None, None),
            P("dp", "expert", None, None),
            P("dp", None, None, None),
            P("dp", None),
            P("dp", "expert", None, None),
            P("dp", "expert", None, None),
            P(),
            P("dp", None, None),
            P("dp", None),
            P("expert", None, None),
            P("expert", None, None),
            P("expert", None, None),
        ),
        out_specs=P("dp", "expert", None, None),
        check_vma=False,
    )
```

```python
import functools

import jax
import jax.numpy as jnp
from jax import lax
from jax.experimental import pallas as pl
from jax.experimental.pallas import tpu as pltpu
from jax.sharding import PartitionSpec as P


score_scale = 192.0 ** (-0.5)
norm_eps = 1e-06


cuts = 2

bf16, f32, i32 = jnp.bfloat16, jnp.float32, jnp.int32
VMEM = pl.BlockSpec(memory_space=pltpu.VMEM)
SMEM = pl.BlockSpec(memory_space=pltpu.SMEM)
ANY = pl.BlockSpec(memory_space=pl.ANY)


def flip(value, mask, size):
    return lax.ppermute(value, "expert", [(i, i ^ mask) for i in range(size)])


def call(body, in_specs, outs, operands, flops=0, scratch=(), limit=16):
    return pl.pallas_call(
        body,
        in_specs=in_specs,
        out_specs=[VMEM] * len(outs),
        out_shape=[jax.ShapeDtypeStruct(s, d) for s, d in outs],
        scratch_shapes=list(scratch),
        compiler_params=pltpu.CompilerParams(vmem_limit_bytes=limit * 1024 * 1024),
        cost_estimate=pl.CostEstimate(flops=flops, bytes_accessed=0, transcendentals=0),
    )(*operands)


def gather_latents(own, size, beside):
    pieces = {0: own}
    quarter = size // 4
    for mask in (2 * quarter, 3 * quarter, quarter):
        pieces[mask] = flip(own, mask, size)
    pieces[3 * quarter], beside = lax.optimization_barrier((pieces[3 * quarter], beside))
    step = quarter // 2
    while step:
        for mask in list(pieces):
            pieces[mask ^ step] = flip(pieces[mask], step, size)
        step //= 2
    return [pieces[m] for m in range(size)], beside


def fetch_weights(w_uv, w_out, core, size):
    dp = lax.axis_size("dp")
    heads = w_uv.shape[0]
    half = heads // 2
    width = w_out.shape[0] // heads
    uv_half = lax.dynamic_slice_in_dim(w_uv, core * half, half, 0)
    out_half = lax.dynamic_slice_in_dim(w_out, core * half * width, half * width, 0)
    parts = [(w_uv, w_out)]
    for turn in range(1, dp):
        source = [((i + turn) % dp, i) for i in range(dp)]
        uv_got = lax.ppermute(uv_half, "dp", source)
        out_got = lax.ppermute(out_half, "dp", source)
        parts.append((uv_got, out_got))
        parts.append((flip(uv_got, 1, size), flip(out_got, 1, size)))
    return parts


def head_order(core, heads):
    dp = lax.axis_size("dp")
    index = lax.axis_index("dp")
    half = heads // 2
    order = [index * heads + h for h in range(heads)]
    for turn in range(1, dp):
        first = ((index + turn) % dp) * heads
        order += [first + core * half + h for h in range(half)]
        order += [first + (1 - core) * half + h for h in range(half)]
    return jnp.stack(order).astype(i32)


def attend_body(size, local_len, seq_count, latent, heads, group, *refs):
    info, queries, memory = refs[:3]
    pieces = refs[3 : 3 + size]
    out, keys, rows = refs[3 + size :]
    seg_len = size * local_len
    total_len = seg_len + memory.shape[0]
    shift = local_len.bit_length() - 1
    index = info[0]
    at = lax.broadcasted_iota(i32, (local_len, total_len), 1)
    row = lax.broadcasted_iota(i32, (local_len, total_len), 0)
    pos = jnp.left_shift(jnp.bitwise_xor(jnp.right_shift(at, shift), index), shift) + jnp.bitwise_and(
        at, local_len - 1
    )
    pos = jnp.where(at < seg_len, pos, -1)
    causal = pos <= index * local_len + row
    for s in range(seq_count):
        cols = pl.ds(s * latent, latent)
        for m in range(size):
            keys[pl.ds(m * local_len, local_len), :] = pieces[m][:, cols]
        keys[pl.ds(seg_len, memory.shape[0]), :] = memory[:, cols]
        bias = jnp.where(causal & (pos < info[2 + size // 2 + s]), 0.0, -jnp.inf)
        bias = jnp.concatenate([bias] * group, axis=0)
        for first in range(0, heads, group):
            for h in range(group):
                rows[pl.ds(h * local_len, local_len), :] = queries[
                    :, pl.ds((s * heads + first + h) * latent, latent)
                ]
            scores = lax.dot_general(
                rows[...], keys[...], (((1,), (1,)), ((), ())), preferred_element_type=f32
            )
            scores = scores * score_scale + bias
            top = jnp.max(scores, axis=1, keepdims=True)
            weights = jnp.exp(scores - top)
            total = jnp.sum(weights, axis=1, keepdims=True)
            got = jnp.dot(weights.astype(bf16), keys[...], preferred_element_type=f32) / total
            got = got.astype(bf16)
            for h in range(group):
                out[pl.ds(s * local_len, local_len), pl.ds((first + h) * latent, latent)] = got[
                    h * local_len : (h + 1) * local_len
                ]


def pack(block, value, capacity):
    lanes = block.shape[1]
    for j in range(value.shape[1] // lanes):
        block[j * capacity : (j + 1) * capacity, :] = value[:capacity, j * lanes : (j + 1) * lanes]


def unpack(rows, at, column, block, capacity):
    lanes = block.shape[1]
    for j in range(block.shape[0] // capacity):
        first = column + j * lanes
        rows[at : at + capacity, first : first + lanes] = block[j * capacity : (j + 1) * capacity, :]


def routes(info, table, top, half, pitch):
    rows = table.shape[0]
    table = table[...]
    names, gates = table[:, :top], table[:, top : 2 * top]
    lane = lax.broadcasted_iota(i32, (rows, half), 1)
    named = jnp.zeros((rows, half), f32)
    weight = jnp.zeros((rows, half), f32)
    for m in range(half):
        hit = names == info[2 + m].astype(f32)
        count = jnp.sum(jnp.where(hit, 1.0, 0.0), axis=1, keepdims=True)
        share = jnp.sum(jnp.where(hit, gates, 0.0), axis=1, keepdims=True)
        named = jnp.where(lane == m, count, named)
        weight = jnp.where(lane == m, share, weight)
    r = lax.broadcasted_iota(i32, (rows, rows), 0)
    c = lax.broadcasted_iota(i32, (rows, rows), 1)
    upto = jnp.where(c <= r, 1.0, 0.0).astype(bf16)
    rank = named * jnp.dot(upto, named.astype(bf16), preferred_element_type=f32)
    wide = half * pitch
    col = lax.broadcasted_iota(i32, (half, wide), 1)
    start = lax.broadcasted_iota(i32, (half, wide), 0) * pitch
    inside = (col >= start) & (col < start + pitch)
    spread = jnp.where(inside, 1.0, 0.0).astype(bf16)
    slot = jnp.sum(jnp.where(inside, col - start + 1, 0), axis=0, keepdims=True).astype(f32)
    rank = jnp.dot(rank.astype(bf16), spread, preferred_element_type=f32)
    weight = jnp.dot(weight.astype(bf16), spread, preferred_element_type=f32)
    place = rank == slot
    return jnp.where(place, 1.0, 0.0).astype(bf16), jnp.where(place, weight, 0.0).astype(bf16)


def routes_body(half, quarter, pitch, top, info, own, side, far, own_place, near_mix, side_place, far_place, far_mix):
    placing, near_mix[...] = routes(info, own, top, half, pitch)
    own_place[...] = placing[:, : quarter * pitch]
    side_place[...], _ = routes(info, side, top, quarter, pitch)
    far_place[...], far_mix[...] = routes(info, far, top, half, pitch)


def place_body(pitch, capacity, cuts, placing, *refs):
    across = (((0,), (0,)), ((), ()))
    rows = jnp.concatenate([r[...] for r in refs[:cuts]], axis=1)
    sent = lax.dot_general(placing[...], rows, across, preferred_element_type=f32).astype(bf16)
    for m, block in enumerate(refs[cuts:]):
        pack(block, sent[m * pitch : (m + 1) * pitch], capacity)


def norm_body(parts, seq_count, latent, *refs):
    order, attended, hidden, gain = refs[:4]
    maps = refs[4 : 4 + 2 * parts]
    residual = refs[4 + 2 * parts]
    chunks = refs[5 + 2 * parts :]
    width = gain.shape[1]
    acc = jnp.concatenate([hidden[:, s * width : (s + 1) * width] for s in range(seq_count)], axis=0).astype(f32)
    slot = 0
    for part in range(parts):
        uv, proj = maps[2 * part], maps[2 * part + 1]
        values = []
        for h in range(uv.shape[0]):
            at = pl.multiple_of(order[slot] * latent, latent)
            got = jnp.dot(attended[:, pl.ds(at, latent)], uv[h], preferred_element_type=f32)
            values.append(got.astype(bf16))
            slot += 1
        acc = acc + jnp.dot(jnp.concatenate(values, axis=1), proj[...], preferred_element_type=f32)
    residual[...] = acc
    mean_square = jnp.mean(acc * acc, axis=1, keepdims=True)
    scaled = (acc * lax.rsqrt(mean_square + norm_eps) * gain[...].astype(f32)).astype(bf16)
    step = width // len(chunks)
    for c, chunk in enumerate(chunks):
        chunk[...] = scaled[:, c * step : (c + 1) * step]


def expert_body(count, pitch, capacity, cuts, gate, up, down, *refs):
    taken = refs[: count * cuts]
    given = refs[count * cuts : -1]
    rows = refs[-1]
    step = rows.shape[1] // cuts
    for c in range(cuts):
        for m in range(count):
            unpack(rows, m * pitch, c * step, taken[c * count + m], capacity)
    across = (((1,), (1,)), ((), ()))
    gate_h = lax.dot_general(rows[...], gate[0], across, preferred_element_type=f32)
    up_h = lax.dot_general(rows[...], up[0], across, preferred_element_type=f32)
    act = (gate_h / (1.0 + jnp.exp(-gate_h)) * up_h).astype(bf16)
    for c in range(cuts):
        out = jnp.dot(act, down[0, :, c * step : (c + 1) * step], preferred_element_type=f32).astype(bf16)
        for m in range(count):
            pack(given[c * count + m], out[m * pitch : (m + 1) * pitch], capacity)


def mix_body(half, pitch, capacity, mixing, *refs):
    taken, out, rows = refs[:half], refs[half], refs[half + 1]
    rows[...] = jnp.zeros(rows.shape, bf16)
    for m in range(half):
        unpack(rows, m * pitch, 0, taken[m], capacity)
    out[...] = jnp.dot(mixing[...], rows[...], preferred_element_type=f32).astype(bf16)


def near_mix_body(half, pitch, capacity, mixing, residual, *refs):
    taken, total, rows = refs[:half], refs[half], refs[half + 1]
    rows[...] = jnp.zeros(rows.shape, bf16)
    for m in range(half):
        unpack(rows, m * pitch, 0, taken[m], capacity)
    total[...] = residual[...] + jnp.dot(mixing[...], rows[...], preferred_element_type=f32)


def last_body(local_len, seq_count, total, *refs):
    others, out = refs[:-1], refs[-1]
    other = jnp.concatenate([o[...] for o in others], axis=1).astype(f32)
    done = (total[...] + other).astype(bf16)
    for s in range(seq_count):
        out[:, s, :] = done[s * local_len : (s + 1) * local_len]


def layer(
    hidden,
    queries,
    latents,
    mem_latents,
    lengths,
    ids,
    gates,
    norm_gain,
    w_uv,
    w_out,
    w_gate,
    w_up,
    w_down,
):
    local_len, seq_count, width = hidden.shape[1:]
    latent = latents.shape[3]
    heads = queries.shape[3] // latent
    rows = local_len * seq_count
    top = ids.shape[3]
    size = lax.axis_size("expert")
    index = lax.axis_index("expert")
    core = index & 1
    half = size // 2
    capacity = min(rows, rows * top // size + 2)
    pitch = -(-capacity // 8) * 8
    lanes = 128
    index_here = index % half
    owners = index - index_here + (index_here ^ jnp.arange(half, dtype=i32))
    info = jnp.concatenate([jnp.stack([index, core]).astype(i32), owners, lengths[0]])

    quarter = half // 2
    parts = fetch_weights(w_uv, w_out, core, size)
    beside = (
        queries[0].reshape(local_len, seq_count * heads * latent),
        hidden[0].reshape(local_len, seq_count * width),
        mem_latents[0].reshape(-1, seq_count * latent),
    )
    own_latents = latents[0].reshape(local_len, seq_count * latent)
    pieces, (query_rows, hidden_rows, memory) = gather_latents(own_latents, size, beside)
    table = jnp.concatenate([ids[0].astype(f32), gates[0].astype(f32)], axis=2)
    table = jnp.transpose(table, (1, 0, 2)).reshape(rows, 2 * top)
    far_table = flip(table, half, size)
    side_table = flip(table, quarter, size)
    wide = half * pitch
    short = quarter * pitch
    own_placing, near_mix, side_placing, far_placing, far_mix = call(
        functools.partial(routes_body, half, quarter, pitch, top),
        [SMEM] + [VMEM] * 3,
        [((rows, short), bf16), ((rows, wide), bf16), ((rows, short), bf16)] + [((rows, wide), bf16)] * 2,
        [info, table, side_table, far_table],
        flops=4 * rows * rows * wide,
    )

    group = max(1, min(heads, 512 // local_len))
    total_len = size * local_len + mem_latents.shape[1]
    (attended,) = call(
        functools.partial(attend_body, size, local_len, seq_count, latent, heads, group),
        [SMEM, VMEM, VMEM] + [VMEM] * size,
        [((rows, heads * latent), bf16)],
        [
            info,
            query_rows,
            memory,
            *pieces,
        ],
        flops=4 * rows * heads * latent * total_len,
        scratch=[pltpu.VMEM((total_len, latent), bf16), pltpu.VMEM((group * local_len, latent), bf16)],
        limit=6 + total_len * 9 // 1024 + size // 8,
    )
    step = width // cuts
    residual, *normed = call(
        functools.partial(norm_body, len(parts), seq_count, latent),
        [SMEM] + [VMEM] * (3 + 2 * len(parts)),
        [((rows, width), f32)] + [((rows, step), bf16)] * cuts,
        [
            head_order(core, w_uv.shape[0]),
            attended,
            hidden_rows,
            norm_gain.reshape(1, width),
            *[w for part in parts for w in part],
        ],
        flops=2 * rows * width * heads * w_uv.shape[2],
    )

    def swap(blocks):
        return [blocks[0]] + [flip(blocks[m], m, size) for m in range(1, len(blocks))]

    def place(placing, chunks):
        count = placing.shape[1] // pitch
        sent = (capacity * sum(c.shape[1] for c in chunks) // lanes, lanes)
        return call(
            functools.partial(place_body, pitch, capacity, len(chunks)),
            [VMEM] * (1 + len(chunks)),
            [(sent, bf16)] * count,
            [placing, *chunks],
            flops=2 * rows * width * wide,
        )

    def experts(blocks, column_cuts):
        count = len(blocks) // column_cuts
        return call(
            functools.partial(expert_body, count, pitch, capacity, column_cuts),
            [VMEM] * (3 + len(blocks)),
            [(b.shape, bf16) for b in blocks],
            [jnp.swapaxes(w_gate, 1, 2), jnp.swapaxes(w_up, 1, 2), w_down, *blocks],
            flops=6 * wide * width * w_gate.shape[2],
            scratch=[pltpu.VMEM((count * pitch, width), bf16)],
        )

    hops = [flip(normed[c], half, size) for c in range(cuts)]
    sides = [flip(normed[c], quarter, size) for c in range(cuts)]
    own_in = swap(place(own_placing, normed))
    side_in = swap(place(side_placing, sides))
    far_in = [swap(place(far_placing, [hops[c]])) for c in range(cuts)]
    own_out = experts(own_in, 1)
    side_out = experts(side_in, 1)
    near_back = [own_out[0]] + [flip(own_out[m], m, size) for m in range(1, quarter)]
    near_back += [flip(side_out[m], m + quarter, size) for m in range(quarter)]
    far_out = experts([b for chunk in far_in for b in chunk], cuts)
    others = []
    for c in range(cuts):
        sent = far_out[c * half : (c + 1) * half]
        got = [sent[0]] + [flip(sent[m], m, size) for m in range(1, quarter)]
        got += [flip(sent[m], m, size) for m in range(quarter, half)]
        (far_sum,) = call(
            functools.partial(mix_body, half, pitch, capacity),
            [VMEM] * (1 + half),
            [((rows, step), bf16)],
            [far_mix, *got],
            flops=2 * rows * step * wide,
            scratch=[pltpu.VMEM((wide, step), bf16)],
        )
        others.append(flip(far_sum, half, size))
    (total,) = call(
        functools.partial(near_mix_body, half, pitch, capacity),
        [VMEM] * (2 + half),
        [((rows, width), f32)],
        [near_mix, residual, *near_back],
        flops=2 * rows * width * wide,
        scratch=[pltpu.VMEM((wide, width), bf16)],
    )
    (out,) = call(
        functools.partial(last_body, local_len, seq_count),
        [VMEM] * (1 + cuts),
        [((local_len, seq_count, width), bf16)],
        [total, *others],
        flops=8 * rows * width,
    )
    return out.reshape(1, local_len, seq_count, width)


def solution(mesh):
    return spread(mesh)


def spread(mesh):
    return jax.shard_map(
        layer,
        mesh=mesh,
        in_specs=(
            P("dp", "expert", None, None),
            P("dp", "expert", None, None),
            P("dp", "expert", None, None),
            P("dp", None, None, None),
            P("dp", None),
            P("dp", "expert", None, None),
            P("dp", "expert", None, None),
            P(),
            P("dp", None, None),
            P("dp", None),
            P("expert", None, None),
            P("expert", None, None),
            P("expert", None, None),
        ),
        out_specs=P("dp", "expert", None, None),
        check_vma=False,
    )
```

```python
import functools

import jax
import jax.numpy as jnp
from jax import lax
from jax.experimental import pallas as pl
from jax.experimental.pallas import tpu as pltpu
from jax.sharding import PartitionSpec as P


score_scale = 192.0 ** (-0.5)
norm_eps = 1e-06


cuts = 2

bf16, f32, i32 = jnp.bfloat16, jnp.float32, jnp.int32
VMEM = pl.BlockSpec(memory_space=pltpu.VMEM)
SMEM = pl.BlockSpec(memory_space=pltpu.SMEM)
ANY = pl.BlockSpec(memory_space=pl.ANY)


def flip(value, mask, size):
    return lax.ppermute(value, "expert", [(i, i ^ mask) for i in range(size)])


def call(body, in_specs, outs, operands, flops=0, scratch=(), limit=16):
    return pl.pallas_call(
        body,
        in_specs=in_specs,
        out_specs=[VMEM] * len(outs),
        out_shape=[jax.ShapeDtypeStruct(s, d) for s, d in outs],
        scratch_shapes=list(scratch),
        compiler_params=pltpu.CompilerParams(vmem_limit_bytes=limit * 1024 * 1024),
        cost_estimate=pl.CostEstimate(flops=flops, bytes_accessed=0, transcendentals=0),
    )(*operands)


def gather_latents(own, size, beside):
    pieces = {0: own}
    quarter = size // 4
    for mask in (2 * quarter, 3 * quarter, quarter):
        pieces[mask] = flip(own, mask, size)
    pieces[3 * quarter], beside = lax.optimization_barrier((pieces[3 * quarter], beside))
    step = quarter // 2
    while step:
        for mask in list(pieces):
            pieces[mask ^ step] = flip(pieces[mask], step, size)
        step //= 2
    return [pieces[m] for m in range(size)], beside


def fetch_weights(w_uv, w_out, core, size):
    dp = lax.axis_size("dp")
    heads = w_uv.shape[0]
    half = heads // 2
    width = w_out.shape[0] // heads
    uv_half = lax.dynamic_slice_in_dim(w_uv, core * half, half, 0)
    out_half = lax.dynamic_slice_in_dim(w_out, core * half * width, half * width, 0)
    parts = [(w_uv, w_out)]
    for turn in range(1, dp):
        source = [((i + turn) % dp, i) for i in range(dp)]
        uv_got = lax.ppermute(uv_half, "dp", source)
        out_got = lax.ppermute(out_half, "dp", source)
        parts.append((uv_got, out_got))
        parts.append((flip(uv_got, 1, size), flip(out_got, 1, size)))
    return parts


def head_order(core, heads):
    dp = lax.axis_size("dp")
    index = lax.axis_index("dp")
    half = heads // 2
    order = [index * heads + h for h in range(heads)]
    for turn in range(1, dp):
        first = ((index + turn) % dp) * heads
        order += [first + core * half + h for h in range(half)]
        order += [first + (1 - core) * half + h for h in range(half)]
    return jnp.stack(order).astype(i32)


def attend_body(size, local_len, seq_count, latent, heads, group, *refs):
    info, queries, memory = refs[:3]
    pieces = refs[3 : 3 + size]
    out, keys, rows = refs[3 + size :]
    seg_len = size * local_len
    total_len = seg_len + memory.shape[0]
    shift = local_len.bit_length() - 1
    index = info[0]
    at = lax.broadcasted_iota(i32, (local_len, total_len), 1)
    row = lax.broadcasted_iota(i32, (local_len, total_len), 0)
    pos = jnp.left_shift(jnp.bitwise_xor(jnp.right_shift(at, shift), index), shift) + jnp.bitwise_and(
        at, local_len - 1
    )
    pos = jnp.where(at < seg_len, pos, -1)
    causal = pos <= index * local_len + row
    for s in range(seq_count):
        cols = pl.ds(s * latent, latent)
        for m in range(size):
            keys[pl.ds(m * local_len, local_len), :] = pieces[m][:, cols]
        keys[pl.ds(seg_len, memory.shape[0]), :] = memory[:, cols]
        bias = jnp.where(causal & (pos < info[2 + size // 2 + s]), 0.0, -jnp.inf)
        bias = jnp.concatenate([bias] * group, axis=0)
        for first in range(0, heads, group):
            for h in range(group):
                rows[pl.ds(h * local_len, local_len), :] = queries[
                    :, pl.ds((s * heads + first + h) * latent, latent)
                ]
            scores = lax.dot_general(
                rows[...], keys[...], (((1,), (1,)), ((), ())), preferred_element_type=f32
            )
            scores = scores * score_scale + bias
            top = jnp.max(scores, axis=1, keepdims=True)
            weights = jnp.exp(scores - top)
            total = jnp.sum(weights, axis=1, keepdims=True)
            got = jnp.dot(weights.astype(bf16), keys[...], preferred_element_type=f32) / total
            got = got.astype(bf16)
            for h in range(group):
                out[pl.ds(s * local_len, local_len), pl.ds((first + h) * latent, latent)] = got[
                    h * local_len : (h + 1) * local_len
                ]


def pack(block, value, capacity):
    lanes = block.shape[1]
    for j in range(value.shape[1] // lanes):
        block[j * capacity : (j + 1) * capacity, :] = value[:capacity, j * lanes : (j + 1) * lanes]


def unpack(rows, at, column, block, capacity):
    lanes = block.shape[1]
    for j in range(block.shape[0] // capacity):
        first = column + j * lanes
        rows[at : at + capacity, first : first + lanes] = block[j * capacity : (j + 1) * capacity, :]


def routes(info, table, top, half, pitch):
    rows = table.shape[0]
    table = table[...]
    names, gates = table[:, :top], table[:, top : 2 * top]
    lane = lax.broadcasted_iota(i32, (rows, half), 1)
    named = jnp.zeros((rows, half), f32)
    weight = jnp.zeros((rows, half), f32)
    for m in range(half):
        hit = names == info[2 + m].astype(f32)
        count = jnp.sum(jnp.where(hit, 1.0, 0.0), axis=1, keepdims=True)
        share = jnp.sum(jnp.where(hit, gates, 0.0), axis=1, keepdims=True)
        named = jnp.where(lane == m, count, named)
        weight = jnp.where(lane == m, share, weight)
    r = lax.broadcasted_iota(i32, (rows, rows), 0)
    c = lax.broadcasted_iota(i32, (rows, rows), 1)
    upto = jnp.where(c <= r, 1.0, 0.0).astype(bf16)
    rank = named * jnp.dot(upto, named.astype(bf16), preferred_element_type=f32)
    wide = half * pitch
    col = lax.broadcasted_iota(i32, (half, wide), 1)
    start = lax.broadcasted_iota(i32, (half, wide), 0) * pitch
    inside = (col >= start) & (col < start + pitch)
    spread = jnp.where(inside, 1.0, 0.0).astype(bf16)
    slot = jnp.sum(jnp.where(inside, col - start + 1, 0), axis=0, keepdims=True).astype(f32)
    rank = jnp.dot(rank.astype(bf16), spread, preferred_element_type=f32)
    weight = jnp.dot(weight.astype(bf16), spread, preferred_element_type=f32)
    place = rank == slot
    return jnp.where(place, 1.0, 0.0).astype(bf16), jnp.where(place, weight, 0.0).astype(bf16)


def routes_body(half, quarter, pitch, top, info, own, side, far, own_place, near_mix, side_place, far_place, far_mix):
    placing, near_mix[...] = routes(info, own, top, half, pitch)
    own_place[...] = placing[:, : quarter * pitch]
    side_place[...], _ = routes(info, side, top, quarter, pitch)
    far_place[...], far_mix[...] = routes(info, far, top, half, pitch)


def place_body(pitch, capacity, cuts, placing, *refs):
    across = (((0,), (0,)), ((), ()))
    rows = jnp.concatenate([r[...] for r in refs[:cuts]], axis=1)
    sent = lax.dot_general(placing[...], rows, across, preferred_element_type=f32).astype(bf16)
    for m, block in enumerate(refs[cuts:]):
        pack(block, sent[m * pitch : (m + 1) * pitch], capacity)


def norm_body(parts, seq_count, latent, *refs):
    order, attended, hidden, gain = refs[:4]
    maps = refs[4 : 4 + 2 * parts]
    residual = refs[4 + 2 * parts]
    chunks = refs[5 + 2 * parts :]
    width = gain.shape[1]
    acc = jnp.concatenate([hidden[:, s * width : (s + 1) * width] for s in range(seq_count)], axis=0).astype(f32)
    slot = 0
    for part in range(parts):
        uv, proj = maps[2 * part], maps[2 * part + 1]
        values = []
        for h in range(uv.shape[0]):
            at = pl.multiple_of(order[slot] * latent, latent)
            got = jnp.dot(attended[:, pl.ds(at, latent)], uv[h], preferred_element_type=f32)
            values.append(got.astype(bf16))
            slot += 1
        acc = acc + jnp.dot(jnp.concatenate(values, axis=1), proj[...], preferred_element_type=f32)
    residual[...] = acc
    mean_square = jnp.mean(acc * acc, axis=1, keepdims=True)
    scaled = (acc * lax.rsqrt(mean_square + norm_eps) * gain[...].astype(f32)).astype(bf16)
    step = width // len(chunks)
    for c, chunk in enumerate(chunks):
        chunk[...] = scaled[:, c * step : (c + 1) * step]


def expert_body(count, pitch, capacity, cuts, gate, up, down, *refs):
    taken = refs[: count * cuts]
    given = refs[count * cuts : -1]
    rows = refs[-1]
    step = rows.shape[1] // cuts
    for c in range(cuts):
        for m in range(count):
            unpack(rows, m * pitch, c * step, taken[c * count + m], capacity)
    across = (((1,), (1,)), ((), ()))
    gate_h = lax.dot_general(rows[...], gate[0], across, preferred_element_type=f32)
    up_h = lax.dot_general(rows[...], up[0], across, preferred_element_type=f32)
    act = (gate_h / (1.0 + jnp.exp(-gate_h)) * up_h).astype(bf16)
    for c in range(cuts):
        out = jnp.dot(act, down[0, :, c * step : (c + 1) * step], preferred_element_type=f32).astype(bf16)
        for m in range(count):
            pack(given[c * count + m], out[m * pitch : (m + 1) * pitch], capacity)


def mix_body(half, pitch, capacity, mixing, *refs):
    taken, out, rows = refs[:half], refs[half], refs[half + 1]
    rows[...] = jnp.zeros(rows.shape, bf16)
    for m in range(half):
        unpack(rows, m * pitch, 0, taken[m], capacity)
    out[...] = jnp.dot(mixing[...], rows[...], preferred_element_type=f32).astype(bf16)


def near_mix_body(half, pitch, capacity, mixing, residual, *refs):
    taken, total, rows = refs[:half], refs[half], refs[half + 1]
    rows[...] = jnp.zeros(rows.shape, bf16)
    for m in range(half):
        unpack(rows, m * pitch, 0, taken[m], capacity)
    total[...] = residual[...] + jnp.dot(mixing[...], rows[...], preferred_element_type=f32)


def last_body(local_len, seq_count, total, *refs):
    others, out = refs[:-1], refs[-1]
    other = jnp.concatenate([o[...] for o in others], axis=1).astype(f32)
    done = (total[...] + other).astype(bf16)
    for s in range(seq_count):
        out[:, s, :] = done[s * local_len : (s + 1) * local_len]


def layer(
    hidden,
    queries,
    latents,
    mem_latents,
    lengths,
    ids,
    gates,
    norm_gain,
    w_uv,
    w_out,
    w_gate,
    w_up,
    w_down,
):
    local_len, seq_count, width = hidden.shape[1:]
    latent = latents.shape[3]
    heads = queries.shape[3] // latent
    rows = local_len * seq_count
    top = ids.shape[3]
    size = lax.axis_size("expert")
    index = lax.axis_index("expert")
    core = index & 1
    half = size // 2
    capacity = min(rows, rows * top // size + 2)
    pitch = -(-capacity // 8) * 8
    lanes = 128
    index_here = index % half
    owners = index - index_here + (index_here ^ jnp.arange(half, dtype=i32))
    info = jnp.concatenate([jnp.stack([index, core]).astype(i32), owners, lengths[0]])

    quarter = half // 2
    parts = fetch_weights(w_uv, w_out, core, size)
    beside = (
        queries[0].reshape(local_len, seq_count * heads * latent),
        hidden[0].reshape(local_len, seq_count * width),
    )
    memory = mem_latents[0].reshape(-1, seq_count * latent)
    own_latents = latents[0].reshape(local_len, seq_count * latent)
    own_latents, memory = lax.optimization_barrier((own_latents, memory))
    pieces, (query_rows, hidden_rows) = gather_latents(own_latents, size, beside)
    table = jnp.concatenate([ids[0].astype(f32), gates[0].astype(f32)], axis=2)
    table = jnp.transpose(table, (1, 0, 2)).reshape(rows, 2 * top)
    far_table = flip(table, half, size)
    side_table = flip(table, quarter, size)
    wide = half * pitch
    short = quarter * pitch
    own_placing, near_mix, side_placing, far_placing, far_mix = call(
        functools.partial(routes_body, half, quarter, pitch, top),
        [SMEM] + [VMEM] * 3,
        [((rows, short), bf16), ((rows, wide), bf16), ((rows, short), bf16)] + [((rows, wide), bf16)] * 2,
        [info, table, side_table, far_table],
        flops=4 * rows * rows * wide,
    )

    group = max(1, min(heads, 512 // local_len))
    total_len = size * local_len + mem_latents.shape[1]
    (attended,) = call(
        functools.partial(attend_body, size, local_len, seq_count, latent, heads, group),
        [SMEM, VMEM, VMEM] + [VMEM] * size,
        [((rows, heads * latent), bf16)],
        [
            info,
            query_rows,
            memory,
            *pieces,
        ],
        flops=4 * rows * heads * latent * total_len,
        scratch=[pltpu.VMEM((total_len, latent), bf16), pltpu.VMEM((group * local_len, latent), bf16)],
        limit=6 + total_len * 9 // 1024 + size // 8,
    )
    step = width // cuts
    residual, *normed = call(
        functools.partial(norm_body, len(parts), seq_count, latent),
        [SMEM] + [VMEM] * (3 + 2 * len(parts)),
        [((rows, width), f32)] + [((rows, step), bf16)] * cuts,
        [
            head_order(core, w_uv.shape[0]),
            attended,
            hidden_rows,
            norm_gain.reshape(1, width),
            *[w for part in parts for w in part],
        ],
        flops=2 * rows * width * heads * w_uv.shape[2],
    )

    def swap(blocks):
        return [blocks[0]] + [flip(blocks[m], m, size) for m in range(1, len(blocks))]

    def place(placing, chunks):
        count = placing.shape[1] // pitch
        sent = (capacity * sum(c.shape[1] for c in chunks) // lanes, lanes)
        return call(
            functools.partial(place_body, pitch, capacity, len(chunks)),
            [VMEM] * (1 + len(chunks)),
            [(sent, bf16)] * count,
            [placing, *chunks],
            flops=2 * rows * width * wide,
        )

    def experts(blocks, column_cuts):
        count = len(blocks) // column_cuts
        return call(
            functools.partial(expert_body, count, pitch, capacity, column_cuts),
            [VMEM] * (3 + len(blocks)),
            [(b.shape, bf16) for b in blocks],
            [jnp.swapaxes(w_gate, 1, 2), jnp.swapaxes(w_up, 1, 2), w_down, *blocks],
            flops=6 * wide * width * w_gate.shape[2],
            scratch=[pltpu.VMEM((count * pitch, width), bf16)],
        )

    hops = [flip(normed[c], half, size) for c in range(cuts)]
    sides = [flip(normed[c], quarter, size) for c in range(cuts)]
    own_in = swap(place(own_placing, normed))
    side_in = swap(place(side_placing, sides))
    far_in = [swap(place(far_placing, [hops[c]])) for c in range(cuts)]
    own_out = experts(own_in, 1)
    side_out = experts(side_in, 1)
    near_back = [own_out[0]] + [flip(own_out[m], m, size) for m in range(1, quarter)]
    near_back += [flip(side_out[m], m + quarter, size) for m in range(quarter)]
    far_out = experts([b for chunk in far_in for b in chunk], cuts)
    others = []
    for c in range(cuts):
        sent = far_out[c * half : (c + 1) * half]
        got = [sent[0]] + [flip(sent[m], m, size) for m in range(1, quarter)]
        got += [flip(sent[m], m, size) for m in range(quarter, half)]
        (far_sum,) = call(
            functools.partial(mix_body, half, pitch, capacity),
            [VMEM] * (1 + half),
            [((rows, step), bf16)],
            [far_mix, *got],
            flops=2 * rows * step * wide,
            scratch=[pltpu.VMEM((wide, step), bf16)],
        )
        others.append(flip(far_sum, half, size))
    (total,) = call(
        functools.partial(near_mix_body, half, pitch, capacity),
        [VMEM] * (2 + half),
        [((rows, width), f32)],
        [near_mix, residual, *near_back],
        flops=2 * rows * width * wide,
        scratch=[pltpu.VMEM((wide, width), bf16)],
    )
    (out,) = call(
        functools.partial(last_body, local_len, seq_count),
        [VMEM] * (1 + cuts),
        [((local_len, seq_count, width), bf16)],
        [total, *others],
        flops=8 * rows * width,
    )
    return out.reshape(1, local_len, seq_count, width)


def solution(mesh):
    return spread(mesh)


def spread(mesh):
    return jax.shard_map(
        layer,
        mesh=mesh,
        in_specs=(
            P("dp", "expert", None, None),
            P("dp", "expert", None, None),
            P("dp", "expert", None, None),
            P("dp", None, None, None),
            P("dp", None),
            P("dp", "expert", None, None),
            P("dp", "expert", None, None),
            P(),
            P("dp", None, None),
            P("dp", None),
            P("expert", None, None),
            P("expert", None, None),
            P("expert", None, None),
        ),
        out_specs=P("dp", "expert", None, None),
        check_vma=False,
    )
```
